128 devices in a mesh: traj: 4 (over y), grid: 32 (over x, z, core).
Axes of the slice: x: 4, y: 4, z: 4, core: 2. Of those that a mesh axis runs over, the one named last changes fastest.
Arguments:
- psi_modes: float32 [4, 2, 256, 256, 256], P('traj', None, None, 'grid'), may hold values from -6 to 6
- noise: float32 [4, 2, 256, 256, 256], P('traj', None, 'grid'), may hold values from -6 to 6
- mask: int32 [256, 256, 256], P(None, 'grid'), may hold values from 0 to 1, as said below
Outputs:
- psi_next: float32 [4, 2, 256, 256, 256], P('traj', None, None, 'grid')
- momentum_hist: float32 [128], replicated
The draws below stay inside these ranges and needn't reach their ends.
Inputs may be any that keep to these rules, and one draw needn't show every extreme that they name: mask is 0 at every mode whose signed third index has magnitude 256/4 or more, and 1 at some mode whose signed third index has magnitude 256/4 - 1.
All inputs are finite; a program needn't handle non-finite values.
Results may differ from the reference program's by a relative error of at most 0.00023.
Values sent between devices are 32-bit elements; how exact they have to be, the bound alone decides.
No kernel may reach another device: no remote copies, remote signals or barrier semaphores. Data moves between devices by JAX's collectives and lax.ppermute only.
A program may use at most 128 MiB of HBM per device.

```python
import jax
import jax.numpy as jnp
from jax import lax

NX = 256
NY = 256
NZ = 256
SHELLS = 128
TRAJ = 4


def signed_range(count):
    index = jnp.arange(count, dtype=jnp.int32)
    return jnp.where(index < count // 2, index, index - count)


def draw_mask(key, part):
    first, second = jax.random.split(jax.random.fold_in(key, 7))
    quarter = NZ // 4
    limit_sq = jax.random.randint(first, (), (quarter - 1) * (quarter - 1), 2 * (quarter - 1) * (quarter - 1) + 1)
    mode_x = signed_range(NX)[:, None, None]
    mode_y = signed_range(NY)[None, :, None]
    mode_z = signed_range(NZ)[None, None, :]
    radius_sq = mode_x * mode_x + mode_y * mode_y + mode_z * mode_z
    holes = jax.random.randint(second, (NX, NY, NZ), 0, 8) > 0
    anchor = (mode_x == 0) & (mode_y == 0)
    inside = (radius_sq <= limit_sq) & (jnp.abs(mode_z) < quarter) & (holes | anchor)
    return jnp.where(inside, 1, 0).astype(jnp.int32)


def shard_levels(rng, shape, cuts, smallest, high):
    factor_of, own = 1.0, jax.random.fold_in(rng, 6)
    for position, shards_of in cuts:
        heights = jnp.exp(jax.random.uniform(jax.random.fold_in(own, position), (shards_of,), jnp.float32, smallest / len(cuts), high / len(cuts)))
        factor_of = factor_of * jnp.repeat(heights, shape[position] // shards_of).reshape([-1 if axis == position else 1 for axis in range(len(shape))])
    return factor_of


def normal_values(key, extent, deviation, most, shards=(), kind=jnp.bfloat16):
    gain = shard_levels(key, extent, shards, -0.22, 0.18) if shards else 1.0
    result = jax.random.normal(key, extent, jnp.float32) * deviation * gain
    return jnp.minimum(jnp.maximum(result, -most), most).astype(kind)


def setup_inputs(seed: int = 0) -> dict:
    key_list = jax.random.split(jax.random.key(seed), 4)
    psi_modes = normal_values(key_list[0], (TRAJ, 2, NX, NY, NZ), 1.0, 6.0, ((0, 4), (3, 32)), jnp.float32)
    noise = normal_values(key_list[1], (TRAJ, 2, NX, NY, NZ), 1.0, 6.0, ((0, 4), (2, 32)), jnp.float32)
    mask = draw_mask(jax.random.fold_in(key_list[3], 71), 0)
    return dict(psi_modes=psi_modes, noise=noise, mask=mask)


time_step = 1.0
damping = 0.05
coupling = 10.0
chem_potential = 1.0
noise_amp = 0.1
trap_strength = 8.0


def signed_modes(count):
    index = jnp.arange(count, dtype=jnp.int32)
    return jnp.where(index < count // 2, index, index - count)


def wave_numbers(count):
    return signed_modes(count).astype(jnp.float32) * (2.0 * jnp.pi / count)


def positions(count):
    return (jnp.arange(count, dtype=jnp.float32) + 0.5) / count - 0.5


def reference(psi_modes, noise, mask):
    wave_x = wave_numbers(NX)
    wave_y = wave_numbers(NY)
    wave_z = wave_numbers(NZ)
    ksq = wave_x[:, None, None] ** 2 + wave_y[None, :, None] ** 2 + wave_z[None, None, :] ** 2
    theta = 0.25 * time_step * ksq
    magnitude = jnp.exp(-damping * theta) * mask.astype(jnp.float32)
    factor = lax.complex(magnitude * jnp.cos(theta), -magnitude * jnp.sin(theta))
    sig_x = signed_modes(NX)
    sig_y = signed_modes(NY)
    sig_z = signed_modes(NZ)
    radius_sq = sig_x[:, None, None] ** 2 + sig_y[None, :, None] ** 2 + sig_z[None, None, :] ** 2
    shells = jnp.minimum(radius_sq * SHELLS // (2 * (NZ // 4) * (NZ // 4)), SHELLS - 1).astype(jnp.int32)
    pos_x = positions(NX)
    pos_y = positions(NY)
    pos_z = positions(NZ)
    potential = trap_strength * (pos_x[:, None, None] ** 2 + pos_y[None, :, None] ** 2 + pos_z[None, None, :] ** 2)

    def per_traj(inputs):
        modes, forcing = inputs
        start = lax.complex(modes[0], modes[1]) * factor
        field = jnp.fft.ifftn(start, norm="ortho")
        density = jnp.real(field) ** 2 + jnp.imag(field) ** 2
        energy = potential + coupling * density - chem_potential
        decay = jnp.exp(-damping * energy * time_step)
        evolve = lax.complex(decay * jnp.cos(energy * time_step), -decay * jnp.sin(energy * time_step))
        moved = field * evolve + noise_amp * lax.complex(forcing[0], forcing[1])
        final = jnp.fft.fftn(moved, norm="ortho") * factor
        occupation = jnp.real(final) ** 2 + jnp.imag(final) ** 2
        partial_hist = jax.ops.segment_sum(occupation.reshape(-1), shells.reshape(-1), num_segments=SHELLS)
        return jnp.stack([jnp.real(final), jnp.imag(final)]), partial_hist

    results, partials = lax.map(per_traj, (psi_modes, noise))
    momentum_hist = jnp.sum(partials, axis=0) * (SHELLS / (TRAJ * NX * NY * NZ))
    return results, momentum_hist
```

```python
import jax
import jax.numpy as jnp
import numpy as np
from jax import lax
from jax.experimental import pallas as pl
from jax.experimental.pallas import tpu as pltpu
from jax.sharding import PartitionSpec as P

SHELLS = 128
N = 256
GRID = 32
LOC = N // GRID
ZM = N // 2
TRAJ = 4

time_step = 1.0
damping = 0.05
coupling = 10.0
chem_potential = 1.0
noise_amp = 0.1
trap_strength = 8.0

F32 = jnp.float32
BF16 = jnp.bfloat16

RESIDUES = sorted({(s * s) % 64 for s in range(64)})

SIN_C = (0.9999999957052124, -0.1666665795268036, 0.008333050198586583, -0.00019809014686181177, 2.6050929465880504e-06)
COS_C = (0.9999999997792474, -0.49999999355360947, 0.0416666361485972, -0.001388836006030289, 2.476009476594345e-05, -2.6050342497228447e-07)
PI_HI = 3.140625
PI_LO = float(np.pi - 3.140625)
TRIG_MAX = 4000.0


def host_tables():
    index = np.arange(N)
    signed = np.where(index < N // 2, index, index - N)
    wave = signed * (2.0 * np.pi / N)
    step = np.exp(-(damping + 1j) * 0.25 * time_step * wave**2)
    phase = np.exp(2j * np.pi * ((index[:, None] * index[None, :]) % N) / N) / np.sqrt(N)
    inverse = phase * step[None, :]
    forward = np.conj(phase) * step[:, None]
    cols = np.concatenate([index[: N // 4], index[3 * N // 4 :]])
    inv_tall = np.concatenate([inverse.real, inverse.imag], 0)
    fwd_tall = np.concatenate([forward.real, forward.imag], 0)
    iz = inverse[:, cols].T
    inv_z = np.block([[iz.real, iz.imag], [-iz.imag, iz.real]])
    fz = forward[cols, :].T
    fwd_z = np.block([[fz.real, fz.imag], [-fz.imag, fz.real]])
    return inv_tall, fwd_tall, inv_z, fwd_z


def halves(table):
    table = np.asarray(table, np.float32)
    high = table.astype(BF16)
    low = (table - high.astype(np.float32)).astype(BF16)
    return jnp.asarray(high), jnp.asarray(low)


def split(value):
    high = value.astype(BF16)
    return high, (value - high.astype(F32)).astype(BF16)


def dot(left, right):
    return jnp.dot(left, right, preferred_element_type=F32)


def dot3(left, right):
    return dot(left[0], right[0]) + dot(left[0], right[1]) + dot(left[1], right[0])


def column_transform(table, real, imag):
    count = real.shape[1]
    both = dot3(table, split(jnp.concatenate([real, imag], axis=1)))
    top, low = both[:N], both[N:]
    return top[:, :count] - low[:, count:], top[:, count:] + low[:, :count]


def select_tiles(values):
    lane = lax.broadcasted_iota(jnp.int32, values.shape[:-1] + (ZM,), values.ndim - 1)
    return jnp.where(lane < ZM // 2, values[..., :ZM], values[..., ZM:])


def first_kernel(psi_ref, mask_ref, hi_ref, lo_ref, out_ref, field):
    keep = select_tiles(mask_ref[...]).astype(F32)
    for part in range(2):
        field[part] = (select_tiles(psi_ref[0, part]) * keep).reshape(N * LOC, ZM)
    table = (hi_ref[...], lo_ref[...])
    for row in range(LOC):
        real, imag = column_transform(
            table, field[0, pl.ds(row, N, stride=LOC), :], field[1, pl.ds(row, N, stride=LOC), :]
        )
        out_ref[pl.ds(row, N, stride=2 * LOC), :] = real
        out_ref[pl.ds(LOC + row, N, stride=2 * LOC), :] = imag


def plane_kernel(
    rank_ref, in_ref, noise_ref, iy_hi, iy_lo, iz_hi, iz_lo, fz_hi, fz_lo, fy_hi, fy_lo, out_ref, base
):
    step = pl.program_id(0)

    @pl.when(step == 0)
    def _():
        shape = (N, N)
        pos_y = (lax.broadcasted_iota(jnp.int32, shape, 0).astype(F32) + 0.5) / N - 0.5
        pos_z = (lax.broadcasted_iota(jnp.int32, shape, 1).astype(F32) + 0.5) / N - 0.5
        base[...] = trap_strength * (pos_y * pos_y + pos_z * pos_z) - chem_potential

    pos_x = ((rank_ref[0] * LOC + step).astype(F32) + 0.5) / N - 0.5
    shift_x = trap_strength * pos_x * pos_x

    real = in_ref[:, 0, 0].reshape(N, ZM)
    imag = in_ref[:, 0, 1].reshape(N, ZM)
    real, imag = column_transform((iy_hi[...], iy_lo[...]), real, imag)
    both = dot3(split(jnp.concatenate([real, imag], axis=1)), (iz_hi[...], iz_lo[...]))
    real, imag = both[:, :N], both[:, N:]
    energy = base[...] + shift_x + coupling * (real * real + imag * imag)
    angle = jnp.minimum(energy * time_step, TRIG_MAX)
    turns = jnp.round(angle * (1.0 / np.pi))
    rest = (angle - turns * PI_HI) - turns * PI_LO
    square = rest * rest
    sine = SIN_C[-1]
    for coef in SIN_C[-2::-1]:
        sine = sine * square + coef
    cosine = COS_C[-1]
    for coef in COS_C[-2::-1]:
        cosine = cosine * square + coef
    half = turns * 0.5
    sign = 1.0 - 4.0 * (half - jnp.floor(half))
    decay = jnp.exp(energy * (-damping * time_step)) * sign
    evo_real = decay * cosine
    evo_imag = decay * (sine * rest)
    moved_real = real * evo_real + imag * evo_imag + noise_amp * noise_ref[0, 0, 0]
    moved_imag = imag * evo_real - real * evo_imag + noise_amp * noise_ref[0, 1, 0]
    both = dot3(split(jnp.concatenate([moved_real, moved_imag], axis=1)), (fz_hi[...], fz_lo[...]))
    real, imag = column_transform((fy_hi[...], fy_lo[...]), both[:, :ZM], both[:, ZM:])
    out_ref[:, 0, 0] = real.reshape(GRID, LOC, ZM)
    out_ref[:, 0, 1] = imag.reshape(GRID, LOC, ZM)


def last_kernel(rank_ref, in_ref, mask_ref, hi_ref, lo_ref, out_ref, hist_ref, keep, field, occ_hi, occ_lo):
    keep[...] = select_tiles(mask_ref[...]).astype(F32).reshape(N * LOC, ZM)
    table = (hi_ref[...], lo_ref[...])
    for row in range(LOC):
        real, imag = column_transform(
            table,
            in_ref[pl.ds(row, N, stride=2 * LOC), :],
            in_ref[pl.ds(LOC + row, N, stride=2 * LOC), :],
        )
        mask = keep[pl.ds(row, N, stride=LOC), :]
        real = real * mask
        imag = imag * mask
        field[0, pl.ds(row, N, stride=LOC), :] = real
        field[1, pl.ds(row, N, stride=LOC), :] = imag
        high, low = split(real * real + imag * imag)
        occ_hi[:, row * ZM : (row + 1) * ZM] = high
        occ_lo[:, row * ZM : (row + 1) * ZM] = low
    lane = lax.broadcasted_iota(jnp.int32, (N, LOC, ZM), 2)
    for part in range(2):
        value = field[part].reshape(N, LOC, ZM)
        out_ref[0, part, :, :, :ZM] = jnp.where(lane < ZM // 2, value, 0.0)
        out_ref[0, part, :, :, ZM:] = jnp.where(lane < ZM // 2, 0.0, value)

    shape = (LOC * ZM, SHELLS)
    place = lax.broadcasted_iota(jnp.int32, shape, 0)
    index_y = rank_ref[0] * LOC + (place >> 7)
    index_z = place & (ZM - 1)
    sig_y = jnp.where(index_y < N // 2, index_y, index_y - N)
    sig_z = jnp.where(index_z < ZM // 2, index_z, index_z - ZM)
    rest = jnp.minimum(sig_y * sig_y + sig_z * sig_z, 64 * (SHELLS - 1))
    gap = rest - 64 * lax.broadcasted_iota(jnp.int32, shape, 1)
    shape = (N, SHELLS)
    index_x = lax.broadcasted_iota(jnp.int32, shape, 0)
    sig_x = jnp.where(index_x < N // 2, index_x, index_x - N)
    square_x = sig_x * sig_x
    residue = square_x & 63
    sums = jnp.zeros(shape, F32)
    for first in range(0, len(RESIDUES), 2):
        pair = RESIDUES[first : first + 2]
        hits = jnp.concatenate(
            [jnp.where((gap >= -r) & (gap < 64 - r), 1.0, 0.0).astype(BF16) for r in pair], axis=1
        )
        found = dot(occ_hi[...], hits) + dot(occ_lo[...], hits)
        for place_of, r in enumerate(pair):
            sums = jnp.where(residue == r, found[:, place_of * SHELLS : (place_of + 1) * SHELLS], sums)
    moves = square_x >> 6
    bins = lax.broadcasted_iota(jnp.int32, shape, 1)
    far = moves >= SHELLS - 1
    over = jnp.where(far, sums, 0.0)
    sums = jnp.where(far, 0.0, sums)
    for bit in range(7):
        width = 1 << bit
        chosen = (moves & width) != 0
        past = chosen & (bins >= SHELLS - width)
        over = over + jnp.where(past, sums, 0.0)
        rolled = jnp.where(bins >= width, pltpu.roll(sums, width, 1), 0.0)
        sums = jnp.where(chosen, rolled, sums)
    total = jnp.sum(sums, axis=0, keepdims=True)
    extra = jnp.sum(jnp.sum(over, axis=0, keepdims=True), axis=1, keepdims=True)
    hist_ref[...] = total + jnp.where(bins[:1] == SHELLS - 1, extra, 0.0)


def params(mib):
    return pltpu.CompilerParams(vmem_limit_bytes=mib * 1024 * 1024)


def whole(shape):
    return pl.BlockSpec(shape, lambda *_: (0,) * len(shape))


def exchange(value):
    return lax.all_to_all(value, "grid", split_axis=0, concat_axis=0, tiled=True)


def summed_over(value, axis):
    copies = jnp.broadcast_to(value, (lax.axis_size(axis), *value.shape))
    return jnp.sum(lax.all_to_all(copies, axis, split_axis=0, concat_axis=0, tiled=True), axis=0)


def shards(psi_modes, noise, mask):
    inv_tall, fwd_tall, inv_z, fwd_z = (halves(table) for table in host_tables())
    rank = lax.axis_index("grid").astype(jnp.int32).reshape(1)
    tall = [whole((2 * N, N))] * 2
    smem = pl.BlockSpec(memory_space=pltpu.SMEM)
    rows = GRID * LOC * 2 * LOC
    message = (GRID, LOC, 2, LOC, ZM)
    sent = pl.pallas_call(
        first_kernel,
        out_shape=jax.ShapeDtypeStruct((rows, ZM), F32),
        grid=(1,),
        in_specs=[whole((1, 2, N, LOC, N)), whole((N, LOC, N)), *tall],
        out_specs=whole((rows, ZM)),
        scratch_shapes=[pltpu.VMEM((2, N * LOC, ZM), F32)],
        compiler_params=params(48),
        name="first",
    )(psi_modes, mask, *inv_tall)
    planes = exchange(sent.reshape(message))
    block = pl.BlockSpec((GRID, 1, 2, LOC, ZM), lambda i: (0, i, 0, 0, 0))
    sent = pl.pallas_call(
        plane_kernel,
        out_shape=jax.ShapeDtypeStruct(message, F32),
        grid=(LOC,),
        in_specs=[
            smem,
            block,
            pl.BlockSpec((1, 2, 1, N, N), lambda i: (0, 0, i, 0, 0)),
            *tall,
            *[whole((N, 2 * N))] * 2,
            *tall,
            *tall,
        ],
        out_specs=block,
        scratch_shapes=[pltpu.VMEM((N, N), F32)],
        compiler_params=params(48),
        name="planes",
    )(rank, planes, noise, *inv_tall, *inv_z, *fwd_z, *fwd_tall)
    rows_in = exchange(sent).reshape(rows, ZM)
    psi_next, hist = pl.pallas_call(
        last_kernel,
        out_shape=(
            jax.ShapeDtypeStruct(psi_modes.shape, F32),
            jax.ShapeDtypeStruct((1, SHELLS), F32),
        ),
        grid=(1,),
        in_specs=[smem, whole((rows, ZM)), whole((N, LOC, N)), *tall],
        out_specs=(whole((1, 2, N, LOC, N)), whole((1, SHELLS))),
        scratch_shapes=[
            pltpu.VMEM((N * LOC, ZM), F32),
            pltpu.VMEM((2, N * LOC, ZM), F32),
            pltpu.VMEM((N, LOC * ZM), BF16),
            pltpu.VMEM((N, LOC * ZM), BF16),
        ],
        compiler_params=params(56),
        name="last",
    )(rank, rows_in, mask, *fwd_tall)
    hist = summed_over(summed_over(hist, "grid"), "traj")
    return psi_next, hist.reshape(SHELLS) * (SHELLS / (TRAJ * N * N * N))


def solution(mesh):
    placed = (
        P("traj", None, None, "grid", None),
        P("traj", None, "grid", None, None),
        P(None, "grid", None),
    )
    return jax.shard_map(
        shards,
        mesh=mesh,
        in_specs=placed,
        out_specs=(P("traj", None, None, "grid", None), P()),
        check_vma=False,
    )
```

```python
import jax
import jax.numpy as jnp
import numpy as np
from jax import lax
from jax.experimental import pallas as pl
from jax.experimental.pallas import tpu as pltpu
from jax.sharding import PartitionSpec as P

SHELLS = 128
N = 256
GRID = 32
LOC = N // GRID
ZM = N // 2
TRAJ = 4
PLANES_MIB = 48
STEP_PLANES = 2

time_step = 1.0
damping = 0.05
coupling = 10.0
chem_potential = 1.0
noise_amp = 0.1
trap_strength = 8.0

F32 = jnp.float32
BF16 = jnp.bfloat16

RESIDUES = sorted({(s * s) % 64 for s in range(64)})
NEAR = 96
GAP_MAX = 100.0

SIN_C = [
    c * np.sqrt(2.0) * np.pi ** (2 * k + 1)
    for k, c in enumerate((0.9999999957052124, -0.1666665795268036, 0.008333050198586583, -0.00019809014686181177, 2.6050929465880504e-06))
]
COS_C = [
    c * np.sqrt(2.0) * np.pi ** (2 * k)
    for k, c in enumerate((0.9999999531318189, -0.49999904875147083, 0.041663574368409804, -0.0013853632426514488, 2.3152375214584864e-05))
]
TURN = time_step / (2.0 * np.pi)
DECAY_LOG2 = -damping * 2.0 * np.pi / np.log(2.0)
AMP_LOG2 = -np.log2(noise_amp)


def host_tables():
    index = np.arange(N)
    signed = np.where(index < N // 2, index, index - N)
    wave = signed * (2.0 * np.pi / N)
    step = np.exp(-(damping + 1j) * 0.25 * time_step * wave**2)
    phase = np.exp(2j * np.pi * ((index[:, None] * index[None, :]) % N) / N) / np.sqrt(N)
    inverse = phase * step[None, :]
    forward = np.conj(phase) * step[:, None]
    cols = np.concatenate([index[: N // 4], index[3 * N // 4 :]])
    inv_tall = np.concatenate([inverse.real, inverse.imag], 0)
    fwd_tall = np.concatenate([forward.real, forward.imag], 0)
    iz = inverse[:, cols].T
    inv_z = np.concatenate([iz.real, -iz.imag, iz.imag, iz.real], 0)
    fz = noise_amp * forward[cols, :].T
    fwd_z = np.block([[fz.real, fz.imag], [-fz.imag, fz.real]])
    return inv_tall, fwd_tall, inv_z, fwd_z


def halves(table):
    table = np.asarray(table, np.float32)
    high = table.astype(BF16)
    low = (table - high.astype(np.float32)).astype(BF16)
    return np.stack([high, low])


def split(value):
    high = value.astype(BF16)
    return high, (value - high.astype(F32)).astype(BF16)


def dot(left, right):
    return jnp.dot(left, right, preferred_element_type=F32)


def dot3(left, right):
    return dot(left[0], right[0]) + dot(left[0], right[1]) + dot(left[1], right[0])


def column_transform(table, real, imag):
    count = real.shape[1]
    both = dot3(table, split(jnp.concatenate([real, imag], axis=1)))
    top, low = both[:N], both[N:]
    return top[:, :count] - low[:, count:], top[:, count:] + low[:, :count]


def select_tiles(values):
    lane = lax.broadcasted_iota(jnp.int32, values.shape[:-1] + (ZM,), values.ndim - 1)
    return jnp.where(lane < ZM // 2, values[..., :ZM], values[..., ZM:])


def polynomial(coefs, square):
    value = coefs[-1]
    for coef in coefs[-2::-1]:
        value = value * square + coef
    return value


def first_kernel(psi_hbm, mask_hbm, table_hbm, out_ref, psi, mask, table_ref, field, sems):
    pieces = 4
    rows = N // pieces
    copies = []
    for piece in range(pieces):
        part = pl.ds(piece * rows, rows)
        copies.append(
            (
                pltpu.make_async_copy(psi_hbm.at[0, :, part], psi.at[:, part], sems.at[0, piece]),
                pltpu.make_async_copy(mask_hbm.at[part], mask.at[part], sems.at[1, piece]),
            )
        )
    tables = [pltpu.make_async_copy(table_hbm.at[pl.ds(0, 2)], table_ref, sems.at[2, 0])]
    for pair in copies:
        for copy in pair:
            copy.start()
    for copy in tables:
        copy.start()
    for piece, pair in enumerate(copies):
        for copy in pair:
            copy.wait()
        part = slice(piece * rows, (piece + 1) * rows)
        keep = select_tiles(mask[part]).astype(F32)
        for half in range(2):
            field[half, piece * rows * LOC : (piece + 1) * rows * LOC] = (
                select_tiles(psi[half, part]) * keep
            ).reshape(rows * LOC, ZM)
    for copy in tables:
        copy.wait()
    table = (table_ref[0], table_ref[1])
    for row in range(LOC):
        real, imag = column_transform(
            table, field[0, pl.ds(row, N, stride=LOC), :], field[1, pl.ds(row, N, stride=LOC), :]
        )
        out_ref[:, 0, row] = real.reshape(GRID, LOC, ZM)
        out_ref[:, 1, row] = imag.reshape(GRID, LOC, ZM)


def plane_kernel(
    rank_ref, in_ref, noise_hbm, tables_hbm, out_ref, base, noise_ref, tables, first_field, second_field, sems
):
    step = pl.program_id(0)
    groups = LOC // STEP_PLANES
    table_copies = [
        pltpu.make_async_copy(tables_hbm.at[part], tables.at[part], sems.at[groups + k])
        for k, part in enumerate((pl.ds(0, 2), pl.ds(2, 2), pl.ds(4, 4)))
    ]

    def noise_copy(group):
        planes = pl.ds(group * STEP_PLANES, STEP_PLANES)
        return pltpu.make_async_copy(noise_hbm.at[0, :, planes], noise_ref.at[:, planes], sems.at[group])

    def to_field(group, field):
        lanes = []
        for inner in range(STEP_PLANES):
            rows = pl.ds(group * STEP_PLANES + inner, LOC, stride=LOC)
            real = jnp.concatenate([in_ref[g, 0, rows, :] for g in range(GRID)], axis=0)
            imag = jnp.concatenate([in_ref[g, 1, rows, :] for g in range(GRID)], axis=0)
            real, imag = column_transform((tables[0], tables[1]), real, imag)
            lanes.append(jnp.concatenate([real, imag], axis=1))
        value = split(jnp.concatenate(lanes, axis=0))
        for part in range(2):
            lines = pl.ds(part * N, N)
            field[part] = dot3(value, (tables[2, lines], tables[3, lines]))

    def from_field(group, field):
        lanes = []
        for inner in range(STEP_PLANES):
            plane = group * STEP_PLANES + inner
            pos_x = ((rank_ref[0] * LOC + plane).astype(F32) + 0.5) / N - 0.5
            shift_x = (TURN * trap_strength) * pos_x * pos_x
            real = field[0, inner * N : (inner + 1) * N]
            imag = field[1, inner * N : (inner + 1) * N]
            turns = (base[...] + shift_x) + (TURN * coupling) * (real * real + imag * imag)
            rest = turns - jnp.round(turns)
            square = rest * rest
            sine = polynomial(SIN_C, square) * rest
            cosine = polynomial(COS_C, square)
            decay = jnp.exp2(turns * DECAY_LOG2 + AMP_LOG2)
            evo_real = decay * (1.0 - sine * sine)
            evo_imag = decay * (sine * cosine)
            moved_real = real * evo_real + imag * evo_imag + noise_ref[0, plane]
            moved_imag = imag * evo_real - real * evo_imag + noise_ref[1, plane]
            lanes.append(jnp.concatenate([moved_real, moved_imag], axis=1))
        value = dot3(split(jnp.concatenate(lanes, axis=0)), (tables[4], tables[5]))
        for inner in range(STEP_PLANES):
            rows = pl.ds(group * STEP_PLANES + inner, LOC, stride=LOC)
            both = value[inner * N : (inner + 1) * N]
            real, imag = column_transform((tables[6], tables[7]), both[:, :ZM], both[:, ZM:])
            for g in range(GRID):
                out_ref[g, 0, rows, :] = real[g * LOC : (g + 1) * LOC]
                out_ref[g, 1, rows, :] = imag[g * LOC : (g + 1) * LOC]

    @pl.when(step == 0)
    def _():
        for copy in table_copies[:2]:
            copy.start()
        noise_copy(0).start()
        table_copies[2].start()
        for later in range(1, groups):
            noise_copy(later).start()
        shape = (N, N)
        pos_y = (lax.broadcasted_iota(jnp.int32, shape, 0).astype(F32) + 0.5) / N - 0.5
        pos_z = (lax.broadcasted_iota(jnp.int32, shape, 1).astype(F32) + 0.5) / N - 0.5
        base[...] = TURN * (trap_strength * (pos_y * pos_y + pos_z * pos_z) - chem_potential)
        for copy in table_copies[:2]:
            copy.wait()
        to_field(0, first_field)
        table_copies[2].wait()

    def both_stages(source, target):
        noise_copy(step - 1).wait()
        from_field(step - 1, source)
        to_field(step, target)

    @pl.when((step > 0) & (step < groups) & (step % 2 == 1))
    def _():
        both_stages(first_field, second_field)

    @pl.when((step > 0) & (step < groups) & (step % 2 == 0))
    def _():
        both_stages(second_field, first_field)

    @pl.when(step == groups)
    def _():
        noise_copy(groups - 1).wait()
        from_field(groups - 1, (first_field, second_field)[(groups - 1) % 2])


def last_kernel(
    rank_ref, in_ref, mask_ref, table_ref, out_hbm, hist_ref, keep, field, occ_hi, occ_lo, sems
):
    keep[...] = select_tiles(mask_ref[...]).astype(F32).reshape(N * LOC, ZM)
    table = (table_ref[0], table_ref[1])
    lines = field.reshape(2, 2, N * LOC, ZM)
    low_lane = lax.broadcasted_iota(jnp.int32, (N, ZM), 1) < ZM // 2
    far = jnp.zeros((8, ZM), F32)
    for row in range(LOC):
        real, imag = column_transform(
            table, in_ref[:, 0, row].reshape(N, ZM), in_ref[:, 1, row].reshape(N, ZM)
        )
        rows = pl.ds(row, N, stride=LOC)
        mask = keep[rows, :]
        real = real * mask
        imag = imag * mask
        for half, value in enumerate((real, imag)):
            lines[half, 0, rows, :] = jnp.where(low_lane, value, 0.0)
            lines[half, 1, rows, :] = jnp.where(low_lane, 0.0, value)
        occupation = real * real + imag * imag
        far = far + jnp.sum(occupation[NEAR : N - NEAR].reshape(-1, 8, ZM), axis=0)
        near = jnp.concatenate([occupation[:NEAR], occupation[N - NEAR :]], axis=0)
        high, low = split(near)
        occ_hi[:, row * ZM : (row + 1) * ZM] = high
        occ_lo[:, row * ZM : (row + 1) * ZM] = low
    copies = [
        pltpu.make_async_copy(
            field.at[half, tile],
            out_hbm.at[0, half, :, :, pl.ds(tile * ZM, ZM)],
            sems.at[half, tile],
        )
        for half in range(2)
        for tile in range(2)
    ]
    for copy in copies:
        copy.start()

    shape = (LOC * ZM, SHELLS)
    place = lax.broadcasted_iota(jnp.int32, shape, 0)
    index_y = rank_ref[0] * LOC + (place >> 7)
    index_z = place & (ZM - 1)
    sig_y = jnp.where(index_y < N // 2, index_y, index_y - N)
    sig_z = jnp.where(index_z < ZM // 2, index_z, index_z - ZM)
    rest = jnp.minimum(sig_y * sig_y + sig_z * sig_z, 64 * (SHELLS - 1))
    gap = (rest - 64 * lax.broadcasted_iota(jnp.int32, shape, 1)).astype(F32)
    gap = jnp.clip(gap, -GAP_MAX, GAP_MAX).astype(BF16)
    count = 2 * NEAR
    shape = (count, SHELLS)
    index_x = lax.broadcasted_iota(jnp.int32, shape, 0)
    sig_x = jnp.where(index_x < NEAR, index_x, index_x - count)
    square_x = sig_x * sig_x
    residue = square_x & 63
    sums = jnp.zeros(shape, F32)
    one = jnp.ones((), BF16)
    zero = jnp.zeros((), BF16)
    for first in range(0, len(RESIDUES), 2):
        pair = RESIDUES[first : first + 2]
        hits = jnp.concatenate(
            [jnp.where(jnp.abs(gap + BF16(r - 31.5)) < BF16(32.0), one, zero) for r in pair], axis=1
        )
        found = dot(occ_hi[...], hits) + dot(occ_lo[...], hits)
        for place_of, r in enumerate(pair):
            sums = jnp.where(residue == r, found[:, place_of * SHELLS : (place_of + 1) * SHELLS], sums)
    moves = square_x >> 6
    bins = lax.broadcasted_iota(jnp.int32, shape, 1)
    beyond = moves >= SHELLS - 1
    over = jnp.where(beyond, sums, 0.0)
    sums = jnp.where(beyond, 0.0, sums)
    for bit in range(7):
        width = 1 << bit
        chosen = (moves & width) != 0
        past = chosen & (bins >= SHELLS - width)
        over = over + jnp.where(past, sums, 0.0)
        rolled = jnp.where(bins >= width, pltpu.roll(sums, width, 1), 0.0)
        sums = jnp.where(chosen, rolled, sums)
    total = jnp.sum(sums, axis=0, keepdims=True)
    extra = jnp.sum(over, axis=0, keepdims=True) + jnp.sum(far, axis=0, keepdims=True)
    extra = jnp.sum(extra, axis=1, keepdims=True)
    hist = total + jnp.where(bins[:1] == SHELLS - 1, extra, 0.0)
    hist_ref[...] = jnp.broadcast_to(hist.reshape(1, 1, SHELLS), (GRID, 1, SHELLS))
    for copy in copies:
        copy.wait()


def params(mib):
    return pltpu.CompilerParams(vmem_limit_bytes=mib * 1024 * 1024)


def whole(shape):
    return pl.BlockSpec(shape, lambda *_: (0,) * len(shape))


def exchange(value):
    return lax.all_to_all(value, "grid", split_axis=0, concat_axis=0, tiled=True)


def shards(psi_modes, noise, mask):
    inv_tall, fwd_tall, inv_z, fwd_z = (halves(table) for table in host_tables())
    tables = jnp.asarray(np.concatenate([inv_tall, inv_z, fwd_z, fwd_tall]))
    rank = lax.axis_index("grid").astype(jnp.int32).reshape(1)
    smem = pl.BlockSpec(memory_space=pltpu.SMEM)
    hbm = pl.BlockSpec(memory_space=pltpu.HBM)
    message = (GRID, 2, LOC, LOC, ZM)
    flat = (GRID, 2, LOC * LOC, ZM)
    sent = pl.pallas_call(
        first_kernel,
        out_shape=jax.ShapeDtypeStruct(message, F32),
        grid=(1,),
        in_specs=[hbm] * 3,
        out_specs=whole(message),
        scratch_shapes=[
            pltpu.VMEM((2, N, LOC, N), F32),
            pltpu.VMEM((N, LOC, N), jnp.int32),
            pltpu.VMEM((2, 2 * N, N), BF16),
            pltpu.VMEM((2, N * LOC, ZM), F32),
            pltpu.SemaphoreType.DMA((3, 4)),
        ],
        compiler_params=params(63),
        name="first",
    )(psi_modes, mask, tables)
    planes = exchange(sent).reshape(flat)
    sent = pl.pallas_call(
        plane_kernel,
        out_shape=jax.ShapeDtypeStruct(flat, F32),
        grid=(LOC // STEP_PLANES + 1,),
        in_specs=[
            smem,
            whole(flat),
            hbm,
            hbm,
        ],
        out_specs=whole(flat),
        scratch_shapes=[
            pltpu.VMEM((N, N), F32),
            pltpu.VMEM((2, LOC, N, N), F32),
            pltpu.VMEM(tables.shape, BF16),
            pltpu.VMEM((2, STEP_PLANES * N, N), F32),
            pltpu.VMEM((2, STEP_PLANES * N, N), F32),
            pltpu.SemaphoreType.DMA((LOC // STEP_PLANES + 3,)),
        ],
        compiler_params=params(PLANES_MIB),
        name="planes",
    )(rank, planes, noise, tables)
    rows_in = exchange(sent).reshape(message)
    psi_next, hist = pl.pallas_call(
        last_kernel,
        out_shape=(
            jax.ShapeDtypeStruct(psi_modes.shape, F32),
            jax.ShapeDtypeStruct((GRID, 1, SHELLS), F32),
        ),
        grid=(1,),
        in_specs=[smem, whole(message), whole((N, LOC, N)), pl.BlockSpec((2, 2 * N, N), lambda i: (3, 0, 0))],
        out_specs=(hbm, whole((GRID, 1, SHELLS))),
        scratch_shapes=[
            pltpu.VMEM((N * LOC, ZM), F32),
            pltpu.VMEM((2, 2, N, LOC, ZM), F32),
            pltpu.VMEM((2 * NEAR, LOC * ZM), BF16),
            pltpu.VMEM((2 * NEAR, LOC * ZM), BF16),
            pltpu.SemaphoreType.DMA((2, 2)),
        ],
        compiler_params=params(24),
        name="last",
    )(rank, rows_in, mask, tables)
    hist = jnp.sum(exchange(hist), axis=0)
    for bit in (1, 2):
        hist = hist + lax.ppermute(hist, "traj", [(t, t ^ bit) for t in range(TRAJ)])
    return psi_next, hist.reshape(SHELLS) * (SHELLS / (TRAJ * N * N * N))


def solution(mesh):
    placed = (
        P("traj", None, None, "grid", None),
        P("traj", None, "grid", None, None),
        P(None, "grid", None),
    )
    return jax.shard_map(
        shards,
        mesh=mesh,
        in_specs=placed,
        out_specs=(P("traj", None, None, "grid", None), P()),
        check_vma=False,
    )
```

```python
import jax
import jax.numpy as jnp
import numpy as np
from jax import lax
from jax.experimental import pallas as pl
from jax.experimental.pallas import tpu as pltpu
from jax.sharding import PartitionSpec as P

SHELLS = 128
N = 256
GRID = 32
LOC = N // GRID
ZM = N // 2
TRAJ = 4
PLANES_MIB = 48
STEP_PLANES = 4

time_step = 1.0
damping = 0.05
coupling = 10.0
chem_potential = 1.0
noise_amp = 0.1
trap_strength = 8.0

F32 = jnp.float32
BF16 = jnp.bfloat16

RESIDUES = sorted({(s * s) % 64 for s in range(64)})
NEAR = 96
GAP_MAX = 100.0

SIN_C = [
    c * np.sqrt(2.0) * np.pi ** (2 * k + 1)
    for k, c in enumerate((0.9999999957052124, -0.1666665795268036, 0.008333050198586583, -0.00019809014686181177, 2.6050929465880504e-06))
]
COS_C = [
    c * np.sqrt(2.0) * np.pi ** (2 * k)
    for k, c in enumerate((0.9999999531318189, -0.49999904875147083, 0.041663574368409804, -0.0013853632426514488, 2.3152375214584864e-05))
]
TURN = time_step / (2.0 * np.pi)
DECAY_LOG2 = -damping * 2.0 * np.pi / np.log(2.0)
AMP_LOG2 = -np.log2(noise_amp)


def host_tables():
    index = np.arange(N)
    signed = np.where(index < N // 2, index, index - N)
    wave = signed * (2.0 * np.pi / N)
    step = np.exp(-(damping + 1j) * 0.25 * time_step * wave**2)
    phase = np.exp(2j * np.pi * ((index[:, None] * index[None, :]) % N) / N) / np.sqrt(N)
    inverse = phase * step[None, :]
    forward = np.conj(phase) * step[:, None]
    cols = np.concatenate([index[: N // 4], index[3 * N // 4 :]])
    inv_tall = np.concatenate([inverse.real, inverse.imag], 0)
    fwd_tall = np.concatenate([forward.real, forward.imag], 0)
    iz = inverse[:, cols].T
    inv_z = np.concatenate([iz.real, -iz.imag, iz.imag, iz.real], 0)
    fz = noise_amp * forward[cols, :].T
    fwd_z = np.block([[fz.real, fz.imag], [-fz.imag, fz.real]])
    return inv_tall, fwd_tall, inv_z, fwd_z


def halves(table):
    table = np.asarray(table, np.float32)
    high = table.astype(BF16)
    low = (table - high.astype(np.float32)).astype(BF16)
    return np.stack([high, low])


def split(value):
    high = value.astype(BF16)
    return high, (value - high.astype(F32)).astype(BF16)


def dot(left, right):
    return jnp.dot(left, right, preferred_element_type=F32)


def dot3(left, right):
    return dot(left[0], right[0]) + dot(left[0], right[1]) + dot(left[1], right[0])


def column_transform(table, real, imag):
    count = real.shape[1]
    both = dot3(table, split(jnp.concatenate([real, imag], axis=1)))
    top, low = both[:N], both[N:]
    return top[:, :count] - low[:, count:], top[:, count:] + low[:, :count]


def select_tiles(values):
    lane = lax.broadcasted_iota(jnp.int32, values.shape[:-1] + (ZM,), values.ndim - 1)
    return jnp.where(lane < ZM // 2, values[..., :ZM], values[..., ZM:])


def polynomial(coefs, square):
    value = coefs[-1]
    for coef in coefs[-2::-1]:
        value = value * square + coef
    return value


def first_kernel(psi_hbm, mask_hbm, table_hbm, out_hbm, psi, mask, table_ref, keep, field, partial, out, sems):
    pieces = 4
    count = N // pieces
    copies = [[], [], []]
    for piece in range(pieces):
        part = pl.ds(piece * count, count)
        copies[0].append(pltpu.make_async_copy(mask_hbm.at[part], mask.at[part], sems.at[0, piece]))
        for half in range(2):
            copies[1 + half].append(
                pltpu.make_async_copy(psi_hbm.at[0, half, part], psi.at[half, part], sems.at[1 + half, piece])
            )
    table_copy = pltpu.make_async_copy(table_hbm.at[pl.ds(0, 2)], table_ref, sems.at[3, 0])
    for pair in zip(*copies[:2]):
        for copy in pair:
            copy.start()
    table_copy.start()
    for copy in copies[2]:
        copy.start()
    table = None
    sent = []
    for half in range(2):
        for piece in range(pieces):
            part = slice(piece * count, (piece + 1) * count)
            lines = slice(piece * count * LOC, (piece + 1) * count * LOC)
            if half == 0:
                copies[0][piece].wait()
                keep[lines] = select_tiles(mask[part]).astype(F32).reshape(count * LOC, ZM)
            copies[1 + half][piece].wait()
            field[half, lines] = select_tiles(psi[half, part]).reshape(count * LOC, ZM) * keep[lines]
        if half == 0:
            table_copy.wait()
            table = (table_ref[0], table_ref[1])
        for pair in range(LOC // 2):
            value = jnp.concatenate(
                [field[half, pl.ds(2 * pair + k, N, stride=LOC), :] for k in range(2)], axis=1
            )
            value = dot3(table, split(value))
            if half == 0:
                partial[pair] = value
            else:
                real = partial[pair, :N] - value[N:]
                imag = partial[pair, N:] + value[:N]
                for k in range(2):
                    lanes = slice(k * ZM, (k + 1) * ZM)
                    out[:, 0, 2 * pair + k] = real[:, lanes].reshape(GRID, LOC, ZM)
                    out[:, 1, 2 * pair + k] = imag[:, lanes].reshape(GRID, LOC, ZM)
                rows = pl.ds(2 * pair, 2)
                sent.append(pltpu.make_async_copy(out.at[:, :, rows], out_hbm.at[:, :, rows], sems.at[4, pair]))
                sent[-1].start()
    for copy in sent:
        copy.wait()


def plane_kernel(
    rank_ref, in_ref, noise_hbm, tables_hbm, out_ref, base, noise_ref, tables, sems
):
    step = pl.program_id(0)
    groups = LOC // STEP_PLANES
    table_copies = [
        pltpu.make_async_copy(tables_hbm.at[part], tables.at[part], sems.at[groups + k])
        for k, part in enumerate((pl.ds(0, 2), pl.ds(2, 2), pl.ds(4, 4)))
    ]

    def noise_copy(group):
        planes = pl.ds(group * STEP_PLANES, STEP_PLANES)
        return pltpu.make_async_copy(noise_hbm.at[0, :, planes], noise_ref.at[:, planes], sems.at[group])

    def to_field(group):
        lanes = []
        for inner in range(STEP_PLANES):
            rows = pl.ds(group * STEP_PLANES + inner, LOC, stride=LOC)
            real = jnp.concatenate([in_ref[g, 0, rows, :] for g in range(GRID)], axis=0)
            imag = jnp.concatenate([in_ref[g, 1, rows, :] for g in range(GRID)], axis=0)
            real, imag = column_transform((tables[0], tables[1]), real, imag)
            lanes.append(jnp.concatenate([real, imag], axis=1))
        value = split(jnp.concatenate(lanes, axis=0))
        parts = (pl.ds(0, N), pl.ds(N, N))
        return [dot3(value, (tables[2, lines], tables[3, lines])) for lines in parts]

    def from_field(group, field):
        lanes = []
        for inner in range(STEP_PLANES):
            plane = group * STEP_PLANES + inner
            pos_x = ((rank_ref[0] * LOC + plane).astype(F32) + 0.5) / N - 0.5
            shift_x = (TURN * trap_strength) * pos_x * pos_x
            real = field[0][inner * N : (inner + 1) * N]
            imag = field[1][inner * N : (inner + 1) * N]
            turns = (base[...] + shift_x) + (TURN * coupling) * (real * real + imag * imag)
            rest = turns - jnp.round(turns)
            square = rest * rest
            sine = polynomial(SIN_C, square) * rest
            cosine = polynomial(COS_C, square)
            decay = jnp.exp2(turns * DECAY_LOG2 + AMP_LOG2)
            evo_real = decay * (1.0 - sine * sine)
            evo_imag = decay * (sine * cosine)
            moved_real = real * evo_real + imag * evo_imag + noise_ref[0, plane]
            moved_imag = imag * evo_real - real * evo_imag + noise_ref[1, plane]
            lanes.append(jnp.concatenate([moved_real, moved_imag], axis=1))
        value = dot3(split(jnp.concatenate(lanes, axis=0)), (tables[4], tables[5]))
        for inner in range(STEP_PLANES):
            rows = pl.ds(group * STEP_PLANES + inner, LOC, stride=LOC)
            both = value[inner * N : (inner + 1) * N]
            real, imag = column_transform((tables[6], tables[7]), both[:, :ZM], both[:, ZM:])
            for g in range(GRID):
                out_ref[g, 0, rows, :] = real[g * LOC : (g + 1) * LOC]
                out_ref[g, 1, rows, :] = imag[g * LOC : (g + 1) * LOC]

    @pl.when(step == 0)
    def _():
        for copy in table_copies[:2]:
            copy.start()
        noise_copy(0).start()
        table_copies[2].start()
        for later in range(1, groups):
            noise_copy(later).start()
        shape = (N, N)
        pos_y = (lax.broadcasted_iota(jnp.int32, shape, 0).astype(F32) + 0.5) / N - 0.5
        pos_z = (lax.broadcasted_iota(jnp.int32, shape, 1).astype(F32) + 0.5) / N - 0.5
        base[...] = TURN * (trap_strength * (pos_y * pos_y + pos_z * pos_z) - chem_potential)
        for copy in table_copies[:2]:
            copy.wait()

    field = to_field(step)
    noise_copy(step).wait()

    @pl.when(step == 0)
    def _():
        table_copies[2].wait()

    from_field(step, field)


def last_kernel(
    rank_ref, in_ref, mask_ref, table_ref, out_hbm, hist_ref, keep, field, occ, sems
):
    keep[...] = select_tiles(mask_ref[...]).astype(F32).reshape(N * LOC, ZM)
    table = (table_ref[0], table_ref[1])
    lines = field.reshape(2, 2, N * LOC, ZM)
    low_lane = lax.broadcasted_iota(jnp.int32, (N, ZM), 1) < ZM // 2
    far = jnp.zeros((8, ZM), F32)
    for row in range(LOC):
        real, imag = column_transform(
            table, in_ref[:, 0, row].reshape(N, ZM), in_ref[:, 1, row].reshape(N, ZM)
        )
        rows = pl.ds(row, N, stride=LOC)
        mask = keep[rows, :]
        real = real * mask
        imag = imag * mask
        for half, value in enumerate((real, imag)):
            lines[half, 0, rows, :] = jnp.where(low_lane, value, 0.0)
            lines[half, 1, rows, :] = jnp.where(low_lane, 0.0, value)
        occupation = real * real + imag * imag
        far = far + jnp.sum(occupation[NEAR : N - NEAR].reshape(-1, 8, ZM), axis=0)
        near = jnp.concatenate([occupation[:NEAR], occupation[N - NEAR :]], axis=0)
        high, low = split(near)
        occ[: 2 * NEAR, row * ZM : (row + 1) * ZM] = high
        occ[2 * NEAR :, row * ZM : (row + 1) * ZM] = low
    copies = [
        pltpu.make_async_copy(
            field.at[half, tile],
            out_hbm.at[0, half, :, :, pl.ds(tile * ZM, ZM)],
            sems.at[half, tile],
        )
        for half in range(2)
        for tile in range(2)
    ]
    for copy in copies:
        copy.start()

    shape = (LOC * ZM, SHELLS)
    place = lax.broadcasted_iota(jnp.int32, shape, 0)
    index_y = rank_ref[0] * LOC + (place >> 7)
    index_z = place & (ZM - 1)
    sig_y = jnp.where(index_y < N // 2, index_y, index_y - N)
    sig_z = jnp.where(index_z < ZM // 2, index_z, index_z - ZM)
    rest = jnp.minimum(sig_y * sig_y + sig_z * sig_z, 64 * (SHELLS - 1))
    gap = (rest - 64 * lax.broadcasted_iota(jnp.int32, shape, 1)).astype(F32)
    gap = jnp.clip(gap, -GAP_MAX, GAP_MAX).astype(BF16)
    count = 2 * NEAR
    shape = (count, SHELLS)
    index_x = lax.broadcasted_iota(jnp.int32, shape, 0)
    sig_x = jnp.where(index_x < NEAR, index_x, index_x - count)
    square_x = sig_x * sig_x
    residue = square_x & 63
    sums = jnp.zeros(shape, F32)
    one = jnp.ones((), BF16)
    zero = jnp.zeros((), BF16)
    for first in range(0, len(RESIDUES), 2):
        pair = RESIDUES[first : first + 2]
        hits = jnp.concatenate(
            [jnp.where(jnp.abs(gap + BF16(r - 31.5)) < BF16(32.0), one, zero) for r in pair], axis=1
        )
        found = dot(occ[...], hits)
        found = found[:count] + found[count:]
        for place_of, r in enumerate(pair):
            sums = jnp.where(residue == r, found[:, place_of * SHELLS : (place_of + 1) * SHELLS], sums)
    moves = square_x >> 6
    bins = lax.broadcasted_iota(jnp.int32, shape, 1)
    beyond = moves >= SHELLS - 1
    over = jnp.where(beyond, sums, 0.0)
    sums = jnp.where(beyond, 0.0, sums)
    for bit in range(7):
        width = 1 << bit
        chosen = (moves & width) != 0
        past = chosen & (bins >= SHELLS - width)
        over = over + jnp.where(past, sums, 0.0)
        rolled = jnp.where(bins >= width, pltpu.roll(sums, width, 1), 0.0)
        sums = jnp.where(chosen, rolled, sums)
    total = jnp.sum(sums, axis=0, keepdims=True)
    extra = jnp.sum(over, axis=0, keepdims=True) + jnp.sum(far, axis=0, keepdims=True)
    extra = jnp.sum(extra, axis=1, keepdims=True)
    hist = total + jnp.where(bins[:1] == SHELLS - 1, extra, 0.0)
    hist_ref[...] = jnp.broadcast_to(hist.reshape(1, 1, SHELLS), (GRID, 1, SHELLS))
    for copy in copies:
        copy.wait()


def params(mib):
    return pltpu.CompilerParams(vmem_limit_bytes=mib * 1024 * 1024)


def whole(shape):
    return pl.BlockSpec(shape, lambda *_: (0,) * len(shape))


def exchange(value):
    return lax.all_to_all(value, "grid", split_axis=0, concat_axis=0, tiled=True)


def shards(psi_modes, noise, mask):
    inv_tall, fwd_tall, inv_z, fwd_z = (halves(table) for table in host_tables())
    tables = jnp.asarray(np.concatenate([inv_tall, inv_z, fwd_z, fwd_tall]))
    rank = lax.axis_index("grid").astype(jnp.int32).reshape(1)
    smem = pl.BlockSpec(memory_space=pltpu.SMEM)
    hbm = pl.BlockSpec(memory_space=pltpu.HBM)
    message = (GRID, 2, LOC, LOC, ZM)
    flat = (GRID, 2, LOC * LOC, ZM)
    sent = pl.pallas_call(
        first_kernel,
        out_shape=jax.ShapeDtypeStruct(message, F32),
        grid=(1,),
        in_specs=[hbm] * 3,
        out_specs=hbm,
        scratch_shapes=[
            pltpu.VMEM((2, N, LOC, N), F32),
            pltpu.VMEM((N, LOC, N), jnp.int32),
            pltpu.VMEM((2, 2 * N, N), BF16),
            pltpu.VMEM((N * LOC, ZM), F32),
            pltpu.VMEM((2, N * LOC, ZM), F32),
            pltpu.VMEM((LOC // 2, 2 * N, 2 * ZM), F32),
            pltpu.VMEM(message, F32),
            pltpu.SemaphoreType.DMA((5, 4)),
        ],
        compiler_params=params(63),
        name="first",
    )(psi_modes, mask, tables)
    planes = exchange(sent).reshape(flat)
    sent = pl.pallas_call(
        plane_kernel,
        out_shape=jax.ShapeDtypeStruct(flat, F32),
        grid=(LOC // STEP_PLANES,),
        in_specs=[
            smem,
            whole(flat),
            hbm,
            hbm,
        ],
        out_specs=whole(flat),
        scratch_shapes=[
            pltpu.VMEM((N, N), F32),
            pltpu.VMEM((2, LOC, N, N), F32),
            pltpu.VMEM(tables.shape, BF16),
            pltpu.SemaphoreType.DMA((LOC // STEP_PLANES + 3,)),
        ],
        compiler_params=params(PLANES_MIB),
        name="planes",
    )(rank, planes, noise, tables)
    rows_in = exchange(sent).reshape(message)
    psi_next, hist = pl.pallas_call(
        last_kernel,
        out_shape=(
            jax.ShapeDtypeStruct(psi_modes.shape, F32),
            jax.ShapeDtypeStruct((GRID, 1, SHELLS), F32),
        ),
        grid=(1,),
        in_specs=[smem, whole(message), whole((N, LOC, N)), pl.BlockSpec((2, 2 * N, N), lambda i: (3, 0, 0))],
        out_specs=(hbm, whole((GRID, 1, SHELLS))),
        scratch_shapes=[
            pltpu.VMEM((N * LOC, ZM), F32),
            pltpu.VMEM((2, 2, N, LOC, ZM), F32),
            pltpu.VMEM((4 * NEAR, LOC * ZM), BF16),
            pltpu.SemaphoreType.DMA((2, 2)),
        ],
        compiler_params=params(24),
        name="last",
    )(rank, rows_in, mask, tables)
    hist = jnp.sum(exchange(hist), axis=0)
    for bit in (1, 2):
        hist = hist + lax.ppermute(hist, "traj", [(t, t ^ bit) for t in range(TRAJ)])
    return psi_next, hist.reshape(SHELLS) * (SHELLS / (TRAJ * N * N * N))


def solution(mesh):
    placed = (
        P("traj", None, None, "grid", None),
        P("traj", None, "grid", None, None),
        P(None, "grid", None),
    )
    return jax.shard_map(
        shards,
        mesh=mesh,
        in_specs=placed,
        out_specs=(P("traj", None, None, "grid", None), P()),
        check_vma=False,
    )
```

```python
import jax
import jax.numpy as jnp
import numpy as np
from jax import lax
from jax.experimental import pallas as pl
from jax.experimental.pallas import tpu as pltpu
from jax.sharding import PartitionSpec as P

SHELLS = 128
N = 256
GRID = 32
LOC = N // GRID
ZM = N // 2
TRAJ = 4
PLANES_MIB = 48
STEP_PLANES = 4

time_step = 1.0
damping = 0.05
coupling = 10.0
chem_potential = 1.0
noise_amp = 0.1
trap_strength = 8.0

F32 = jnp.float32
BF16 = jnp.bfloat16

RESIDUES = sorted({(s * s) % 64 for s in range(64)})
NEAR = 96
GAP_MAX = 100.0

SIN_C = [
    c * np.sqrt(2.0) * np.pi ** (2 * k + 1)
    for k, c in enumerate((0.9999999957052124, -0.1666665795268036, 0.008333050198586583, -0.00019809014686181177, 2.6050929465880504e-06))
]
COS_C = [
    c * np.sqrt(2.0) * np.pi ** (2 * k)
    for k, c in enumerate((0.9999999531318189, -0.49999904875147083, 0.041663574368409804, -0.0013853632426514488, 2.3152375214584864e-05))
]
TURN = time_step / (2.0 * np.pi)
DECAY_LOG2 = -damping * 2.0 * np.pi / np.log(2.0)
AMP_LOG2 = -np.log2(noise_amp)


def host_tables():
    index = np.arange(N)
    signed = np.where(index < N // 2, index, index - N)
    wave = signed * (2.0 * np.pi / N)
    step = np.exp(-(damping + 1j) * 0.25 * time_step * wave**2)
    phase = np.exp(2j * np.pi * ((index[:, None] * index[None, :]) % N) / N) / np.sqrt(N)
    inverse = phase * step[None, :]
    forward = np.conj(phase) * step[:, None]
    cols = np.concatenate([index[: N // 4], index[3 * N // 4 :]])
    inv_tall = np.concatenate([inverse.real, inverse.imag], 0)
    fwd_tall = np.concatenate([forward.real, forward.imag], 0)
    iz = inverse[:, cols].T
    inv_z = np.concatenate([iz.real, -iz.imag, iz.imag, iz.real], 0)
    fz = noise_amp * forward[cols, :].T
    fwd_z = np.block([[fz.real, fz.imag], [-fz.imag, fz.real]])
    return inv_tall, fwd_tall, inv_z, fwd_z


def halves(table):
    table = np.asarray(table, np.float32)
    high = table.astype(BF16)
    low = (table - high.astype(np.float32)).astype(BF16)
    return np.stack([high, low])


def split(value):
    high = value.astype(BF16)
    return high, (value - high.astype(F32)).astype(BF16)


def dot(left, right):
    return jnp.dot(left, right, preferred_element_type=F32)


def dot3(left, right):
    return dot(left[0], right[0]) + dot(left[0], right[1]) + dot(left[1], right[0])


def column_transform(table, real, imag):
    count = real.shape[1]
    both = dot3(table, split(jnp.concatenate([real, imag], axis=1)))
    top, low = both[:N], both[N:]
    return top[:, :count] - low[:, count:], top[:, count:] + low[:, :count]


def select_tiles(values):
    lane = lax.broadcasted_iota(jnp.int32, values.shape[:-1] + (ZM,), values.ndim - 1)
    return jnp.where(lane < ZM // 2, values[..., :ZM], values[..., ZM:])


def polynomial(coefs, square):
    value = coefs[-1]
    for coef in coefs[-2::-1]:
        value = value * square + coef
    return value


def first_kernel(psi_hbm, mask_hbm, table_hbm, out_hbm, psi, mask, table_ref, keep, field, partial, out, sems):
    pieces = 4
    count = N // pieces
    copies = [[], [], []]
    for piece in range(pieces):
        part = pl.ds(piece * count, count)
        copies[0].append(pltpu.make_async_copy(mask_hbm.at[part], mask.at[part], sems.at[0, piece]))
        for half in range(2):
            copies[1 + half].append(
                pltpu.make_async_copy(psi_hbm.at[0, half, part], psi.at[half, part], sems.at[1 + half, piece])
            )
    table_copy = pltpu.make_async_copy(table_hbm.at[pl.ds(0, 2)], table_ref, sems.at[3, 0])
    for pair in zip(*copies[:2]):
        for copy in pair:
            copy.start()
    table_copy.start()
    for copy in copies[2]:
        copy.start()
    table = None
    sent = []
    for half in range(2):
        for piece in range(pieces):
            part = slice(piece * count, (piece + 1) * count)
            lines = slice(piece * count * LOC, (piece + 1) * count * LOC)
            if half == 0:
                copies[0][piece].wait()
                keep[lines] = select_tiles(mask[part]).astype(F32).reshape(count * LOC, ZM)
            copies[1 + half][piece].wait()
            field[half, lines] = select_tiles(psi[half, part]).reshape(count * LOC, ZM) * keep[lines]
        if half == 0:
            table_copy.wait()
            table = (table_ref[0], table_ref[1])
        for pair in range(LOC // 2):
            value = jnp.concatenate(
                [field[half, pl.ds(2 * pair + k, N, stride=LOC), :] for k in range(2)], axis=1
            )
            value = dot3(table, split(value))
            if half == 0:
                partial[pair] = value
            else:
                real = partial[pair, :N] - value[N:]
                imag = partial[pair, N:] + value[:N]
                for k in range(2):
                    lanes = slice(k * ZM, (k + 1) * ZM)
                    out[:, 0, 2 * pair + k] = real[:, lanes].reshape(GRID, LOC, ZM)
                    out[:, 1, 2 * pair + k] = imag[:, lanes].reshape(GRID, LOC, ZM)
                rows = pl.ds(2 * pair, 2)
                sent.append(pltpu.make_async_copy(out.at[:, :, rows], out_hbm.at[:, :, rows], sems.at[4, pair]))
                sent[-1].start()
    for copy in sent:
        copy.wait()


def plane_kernel(
    rank_ref, in_ref, noise_hbm, tables_hbm, out_ref, base, noise_ref, tables, sems
):
    step = pl.program_id(0)
    groups = LOC // STEP_PLANES
    table_copies = [
        pltpu.make_async_copy(tables_hbm.at[part], tables.at[part], sems.at[groups + k])
        for k, part in enumerate((pl.ds(0, 2), pl.ds(2, 2), pl.ds(4, 4)))
    ]

    def noise_copy(group):
        planes = pl.ds(group * STEP_PLANES, STEP_PLANES)
        return pltpu.make_async_copy(noise_hbm.at[0, :, planes], noise_ref.at[:, planes], sems.at[group])

    def to_field(group):
        lanes = []
        for inner in range(STEP_PLANES):
            rows = pl.ds(group * STEP_PLANES + inner, LOC, stride=LOC)
            real = jnp.concatenate([in_ref[g, 0, rows, :] for g in range(GRID)], axis=0)
            imag = jnp.concatenate([in_ref[g, 1, rows, :] for g in range(GRID)], axis=0)
            real, imag = column_transform((tables[0], tables[1]), real, imag)
            lanes.append(jnp.concatenate([real, imag], axis=1))
        value = split(jnp.concatenate(lanes, axis=0))
        parts = (pl.ds(0, N), pl.ds(N, N))
        return [dot3(value, (tables[2, lines], tables[3, lines])) for lines in parts]

    def from_field(group, field):
        lanes = []
        for inner in range(STEP_PLANES):
            plane = group * STEP_PLANES + inner
            pos_x = ((rank_ref[0] * LOC + plane).astype(F32) + 0.5) / N - 0.5
            shift_x = (TURN * trap_strength) * pos_x * pos_x
            real = field[0][inner * N : (inner + 1) * N]
            imag = field[1][inner * N : (inner + 1) * N]
            turns = (base[...] + shift_x) + (TURN * coupling) * (real * real + imag * imag)
            rest = turns - jnp.round(turns)
            square = rest * rest
            sine = polynomial(SIN_C, square) * rest
            cosine = polynomial(COS_C, square)
            decay = jnp.exp2(turns * DECAY_LOG2 + AMP_LOG2)
            evo_real = decay * (1.0 - sine * sine)
            evo_imag = decay * (sine * cosine)
            moved_real = real * evo_real + imag * evo_imag + noise_ref[0, plane]
            moved_imag = imag * evo_real - real * evo_imag + noise_ref[1, plane]
            lanes.append(jnp.concatenate([moved_real, moved_imag], axis=1))
        value = dot3(split(jnp.concatenate(lanes, axis=0)), (tables[4], tables[5]))
        for inner in range(STEP_PLANES):
            rows = pl.ds(group * STEP_PLANES + inner, LOC, stride=LOC)
            both = value[inner * N : (inner + 1) * N]
            real, imag = column_transform((tables[6], tables[7]), both[:, :ZM], both[:, ZM:])
            for g in range(GRID):
                out_ref[g, 0, rows, :] = real[g * LOC : (g + 1) * LOC]
                out_ref[g, 1, rows, :] = imag[g * LOC : (g + 1) * LOC]

    @pl.when(step == 0)
    def _():
        for copy in table_copies[:2]:
            copy.start()
        noise_copy(0).start()
        table_copies[2].start()
        for later in range(1, groups):
            noise_copy(later).start()
        shape = (N, N)
        pos_y = (lax.broadcasted_iota(jnp.int32, shape, 0).astype(F32) + 0.5) / N - 0.5
        pos_z = (lax.broadcasted_iota(jnp.int32, shape, 1).astype(F32) + 0.5) / N - 0.5
        base[...] = TURN * (trap_strength * (pos_y * pos_y + pos_z * pos_z) - chem_potential)
        for copy in table_copies[:2]:
            copy.wait()

    field = to_field(step)
    noise_copy(step).wait()

    @pl.when(step == 0)
    def _():
        table_copies[2].wait()

    from_field(step, field)


def last_kernel(
    rank_ref, in_ref, mask_ref, table_ref, out_hbm, hist_ref, keep, field, occ, halves_ref, sems
):
    keep[...] = select_tiles(mask_ref[...]).astype(F32).reshape(N * LOC, ZM)
    lines = field.reshape(2, 2, N * LOC, ZM)
    half_rows = N // 2
    low_lane = lax.broadcasted_iota(jnp.int32, (half_rows, ZM), 1) < ZM // 2
    far = jnp.zeros((8, ZM), F32)
    mirror = lax.broadcasted_iota(jnp.int32, (NEAR, ZM), 1)
    low_near = mirror < ZM // 2
    mirror = jnp.where((mirror & (ZM // 2 - 1)) == 0, ZM // 2 - mirror, ZM - mirror)
    copies = []
    for upper in range(2):
        first = upper * half_rows
        table = tuple(
            jnp.concatenate(
                [table_ref[k, first : first + half_rows], table_ref[k, N + first : N + first + half_rows]], axis=0
            )
            for k in range(2)
        )
        even = None
        for row in range(LOC):
            if upper == 0:
                value = jnp.concatenate(
                    [in_ref[:, 0, row].reshape(N, ZM), in_ref[:, 1, row].reshape(N, ZM)], axis=1
                )
                held = split(value)
                halves_ref[row, 0] = held[0]
                halves_ref[row, 1] = held[1]
            else:
                held = halves_ref[row, 0], halves_ref[row, 1]
            both = dot3(table, held)
            real = both[:half_rows, :ZM] - both[half_rows:, ZM:]
            imag = both[:half_rows, ZM:] + both[half_rows:, :ZM]
            rows = pl.ds(first * LOC + row, half_rows, stride=LOC)
            mask = keep[rows, :]
            real = real * mask
            imag = imag * mask
            for half, value in enumerate((real, imag)):
                lines[half, 0, rows, :] = jnp.where(low_lane, value, 0.0)
                lines[half, 1, rows, :] = jnp.where(low_lane, 0.0, value)
            occupation = real * real + imag * imag
            if upper == 0:
                near, rest = occupation[:NEAR], occupation[NEAR:]
            else:
                rest, near = occupation[: half_rows - NEAR], occupation[half_rows - NEAR :]
            far = far + jnp.sum(rest.reshape(-1, 8, ZM), axis=0)
            if row % 2 == 0:
                even = near
                continue
            folded = jnp.where(low_near, even, near) + jnp.take_along_axis(
                jnp.where(low_near, near, even), mirror, axis=1, mode="promise_in_bounds"
            )
            high, low = split(folded)
            lanes = slice(row // 2 * ZM, (row // 2 + 1) * ZM)
            occ[upper * NEAR : (upper + 1) * NEAR, lanes] = high
            occ[(2 + upper) * NEAR : (3 + upper) * NEAR, lanes] = low
        part = pl.ds(first, half_rows)
        for half in range(2):
            for tile in range(2):
                copies.append(
                    pltpu.make_async_copy(
                        field.at[half, tile, part],
                        out_hbm.at[0, half, part, :, pl.ds(tile * ZM, ZM)],
                        sems.at[half, 2 * upper + tile],
                    )
                )
                copies[-1].start()

    shape = (LOC * ZM // 2, SHELLS)
    place = lax.broadcasted_iota(jnp.int32, shape, 0)
    lane = place & (ZM - 1)
    index_y = rank_ref[0] * LOC + 2 * (place >> 7) + (lane >> 6)
    sig_y = jnp.where(index_y < N // 2, index_y, index_y - N)
    sig_z = jnp.where(lane < ZM // 2, lane, (ZM - lane) & (ZM // 2 - 1))
    rest = jnp.minimum(sig_y * sig_y + sig_z * sig_z, 64 * (SHELLS - 1))
    gap = (rest - 64 * lax.broadcasted_iota(jnp.int32, shape, 1)).astype(F32)
    gap = jnp.clip(gap, -GAP_MAX, GAP_MAX).astype(BF16)
    count = 2 * NEAR
    shape = (count, SHELLS)
    index_x = lax.broadcasted_iota(jnp.int32, shape, 0)
    sig_x = jnp.where(index_x < NEAR, index_x, index_x - count)
    square_x = sig_x * sig_x
    residue = square_x & 63
    sums = jnp.zeros(shape, F32)
    one = jnp.ones((), BF16)
    zero = jnp.zeros((), BF16)
    for first in range(0, len(RESIDUES), 2):
        pair = RESIDUES[first : first + 2]
        hits = jnp.concatenate(
            [jnp.where(jnp.abs(gap + BF16(r - 31.5)) < BF16(32.0), one, zero) for r in pair], axis=1
        )
        found = dot(occ[...], hits)
        found = found[:count] + found[count:]
        for place_of, r in enumerate(pair):
            sums = jnp.where(residue == r, found[:, place_of * SHELLS : (place_of + 1) * SHELLS], sums)
    moves = square_x >> 6
    bins = lax.broadcasted_iota(jnp.int32, shape, 1)
    beyond = moves >= SHELLS - 1
    over = jnp.where(beyond, sums, 0.0)
    sums = jnp.where(beyond, 0.0, sums)
    for bit in range(7):
        width = 1 << bit
        chosen = (moves & width) != 0
        past = chosen & (bins >= SHELLS - width)
        over = over + jnp.where(past, sums, 0.0)
        rolled = jnp.where(bins >= width, pltpu.roll(sums, width, 1), 0.0)
        sums = jnp.where(chosen, rolled, sums)
    total = jnp.sum(sums, axis=0, keepdims=True)
    extra = jnp.sum(over, axis=0, keepdims=True) + jnp.sum(far, axis=0, keepdims=True)
    extra = jnp.sum(extra, axis=1, keepdims=True)
    hist = total + jnp.where(bins[:1] == SHELLS - 1, extra, 0.0)
    hist_ref[...] = jnp.broadcast_to(hist.reshape(1, 1, SHELLS), (GRID, 1, SHELLS))
    for copy in copies:
        copy.wait()


def params(mib):
    return pltpu.CompilerParams(vmem_limit_bytes=mib * 1024 * 1024)


def whole(shape):
    return pl.BlockSpec(shape, lambda *_: (0,) * len(shape))


def exchange(value):
    return lax.all_to_all(value, "grid", split_axis=0, concat_axis=0, tiled=True)


def shards(psi_modes, noise, mask):
    inv_tall, fwd_tall, inv_z, fwd_z = (halves(table) for table in host_tables())
    tables = jnp.asarray(np.concatenate([inv_tall, inv_z, fwd_z, fwd_tall]))
    rank = lax.axis_index("grid").astype(jnp.int32).reshape(1)
    smem = pl.BlockSpec(memory_space=pltpu.SMEM)
    hbm = pl.BlockSpec(memory_space=pltpu.HBM)
    message = (GRID, 2, LOC, LOC, ZM)
    flat = (GRID, 2, LOC * LOC, ZM)
    sent = pl.pallas_call(
        first_kernel,
        out_shape=jax.ShapeDtypeStruct(message, F32),
        grid=(1,),
        in_specs=[hbm] * 3,
        out_specs=hbm,
        scratch_shapes=[
            pltpu.VMEM((2, N, LOC, N), F32),
            pltpu.VMEM((N, LOC, N), jnp.int32),
            pltpu.VMEM((2, 2 * N, N), BF16),
            pltpu.VMEM((N * LOC, ZM), F32),
            pltpu.VMEM((2, N * LOC, ZM), F32),
            pltpu.VMEM((LOC // 2, 2 * N, 2 * ZM), F32),
            pltpu.VMEM(message, F32),
            pltpu.SemaphoreType.DMA((5, 4)),
        ],
        compiler_params=params(63),
        name="first",
    )(psi_modes, mask, tables)
    planes = exchange(sent).reshape(flat)
    sent = pl.pallas_call(
        plane_kernel,
        out_shape=jax.ShapeDtypeStruct(flat, F32),
        grid=(LOC // STEP_PLANES,),
        in_specs=[
            smem,
            whole(flat),
            hbm,
            hbm,
        ],
        out_specs=whole(flat),
        scratch_shapes=[
            pltpu.VMEM((N, N), F32),
            pltpu.VMEM((2, LOC, N, N), F32),
            pltpu.VMEM(tables.shape, BF16),
            pltpu.SemaphoreType.DMA((LOC // STEP_PLANES + 3,)),
        ],
        compiler_params=params(PLANES_MIB),
        name="planes",
    )(rank, planes, noise, tables)
    rows_in = exchange(sent).reshape(message)
    psi_next, hist = pl.pallas_call(
        last_kernel,
        out_shape=(
            jax.ShapeDtypeStruct(psi_modes.shape, F32),
            jax.ShapeDtypeStruct((GRID, 1, SHELLS), F32),
        ),
        grid=(1,),
        in_specs=[smem, whole(message), whole((N, LOC, N)), pl.BlockSpec((2, 2 * N, N), lambda i: (3, 0, 0))],
        out_specs=(hbm, whole((GRID, 1, SHELLS))),
        scratch_shapes=[
            pltpu.VMEM((N * LOC, ZM), F32),
            pltpu.VMEM((2, 2, N, LOC, ZM), F32),
            pltpu.VMEM((4 * NEAR, LOC * ZM // 2), BF16),
            pltpu.VMEM((LOC, 2, N, 2 * ZM), BF16),
            pltpu.SemaphoreType.DMA((2, 4)),
        ],
        compiler_params=params(24),
        name="last",
    )(rank, rows_in, mask, tables)
    hist = jnp.sum(exchange(hist), axis=0)
    for bit in (1, 2):
        hist = hist + lax.ppermute(hist, "traj", [(t, t ^ bit) for t in range(TRAJ)])
    return psi_next, hist.reshape(SHELLS) * (SHELLS / (TRAJ * N * N * N))


def solution(mesh):
    placed = (
        P("traj", None, None, "grid", None),
        P("traj", None, "grid", None, None),
        P(None, "grid", None),
    )
    return jax.shard_map(
        shards,
        mesh=mesh,
        in_specs=placed,
        out_specs=(P("traj", None, None, "grid", None), P()),
        check_vma=False,
    )
```

```python
import jax
import jax.numpy as jnp
import numpy as np
from jax import lax
from jax.experimental import pallas as pl
from jax.experimental.pallas import tpu as pltpu
from jax.sharding import PartitionSpec as P

SHELLS = 128
N = 256
GRID = 32
LOC = N // GRID
ZM = N // 2
TRAJ = 4
PLANES_MIB = 48
STEP_PLANES = 4

time_step = 1.0
damping = 0.05
coupling = 10.0
chem_potential = 1.0
noise_amp = 0.1
trap_strength = 8.0

F32 = jnp.float32
BF16 = jnp.bfloat16

RESIDUES = sorted({(s * s) % 64 for s in range(64)})
NEAR = 96
GAP_MAX = 100.0

SIN_C = [
    c * np.sqrt(2.0) * np.pi ** (2 * k + 1)
    for k, c in enumerate((0.9999999957052124, -0.1666665795268036, 0.008333050198586583, -0.00019809014686181177, 2.6050929465880504e-06))
]
COS_C = [
    c * np.sqrt(2.0) * np.pi ** (2 * k)
    for k, c in enumerate((0.9999999531318189, -0.49999904875147083, 0.041663574368409804, -0.0013853632426514488, 2.3152375214584864e-05))
]
TURN = time_step / (2.0 * np.pi)
DECAY_LOG2 = -damping * 2.0 * np.pi / np.log(2.0)
AMP_LOG2 = -np.log2(noise_amp)


def host_tables():
    index = np.arange(N)
    signed = np.where(index < N // 2, index, index - N)
    wave = signed * (2.0 * np.pi / N)
    step = np.exp(-(damping + 1j) * 0.25 * time_step * wave**2)
    phase = np.exp(2j * np.pi * ((index[:, None] * index[None, :]) % N) / N) / np.sqrt(N)
    inverse = phase * step[None, :]
    forward = np.conj(phase) * step[:, None]
    cols = np.concatenate([index[: N // 4], index[3 * N // 4 :]])
    inv_tall = np.concatenate([inverse.real, inverse.imag], 0)
    fwd_tall = np.concatenate([forward.real, forward.imag], 0)
    iz = inverse[:, cols].T
    inv_z = np.concatenate([iz.real, -iz.imag, iz.imag, iz.real], 0)
    fz = noise_amp * forward[cols, :].T
    fwd_z = np.block([[fz.real, fz.imag], [-fz.imag, fz.real]])
    return inv_tall, fwd_tall, inv_z, fwd_z


def halves(table):
    table = np.asarray(table, np.float32)
    high = table.astype(BF16)
    low = (table - high.astype(np.float32)).astype(BF16)
    return np.stack([high, low])


def split(value):
    high = value.astype(BF16)
    return high, (value - high.astype(F32)).astype(BF16)


def dot(left, right):
    return jnp.dot(left, right, preferred_element_type=F32)


def dot3(left, right):
    return dot(left[0], right[0]) + dot(left[0], right[1]) + dot(left[1], right[0])


def column_transform(table, real, imag):
    count = real.shape[1]
    both = dot3(table, split(jnp.concatenate([real, imag], axis=1)))
    top, low = both[:N], both[N:]
    return top[:, :count] - low[:, count:], top[:, count:] + low[:, :count]


def select_tiles(values):
    lane = lax.broadcasted_iota(jnp.int32, values.shape[:-1] + (ZM,), values.ndim - 1)
    return jnp.where(lane < ZM // 2, values[..., :ZM], values[..., ZM:])


def polynomial(coefs, square):
    value = coefs[-1]
    for coef in coefs[-2::-1]:
        value = value * square + coef
    return value


def first_kernel(psi_hbm, mask_hbm, table_hbm, out_hbm, psi, mask, table_ref, keep, field, partial, out, sems):
    pieces = 4
    count = N // pieces
    copies = [[], [], []]
    for piece in range(pieces):
        part = pl.ds(piece * count, count)
        copies[0].append(pltpu.make_async_copy(mask_hbm.at[part], mask.at[part], sems.at[0, piece]))
        for half in range(2):
            copies[1 + half].append(
                pltpu.make_async_copy(psi_hbm.at[0, half, part], psi.at[half, part], sems.at[1 + half, piece])
            )
    table_copy = pltpu.make_async_copy(table_hbm.at[pl.ds(0, 2)], table_ref, sems.at[3, 0])
    for pair in zip(*copies[:2]):
        for copy in pair:
            copy.start()
    table_copy.start()
    table = None
    sent = []
    for half in range(2):
        for piece in range(pieces):
            part = slice(piece * count, (piece + 1) * count)
            lines = slice(piece * count * LOC, (piece + 1) * count * LOC)
            if half == 0:
                copies[0][piece].wait()
                keep[lines] = select_tiles(mask[part]).astype(F32).reshape(count * LOC, ZM)
            copies[1 + half][piece].wait()
            if half == 0:
                copies[2][piece].start()
            field[half, lines] = select_tiles(psi[half, part]).reshape(count * LOC, ZM) * keep[lines]
        if half == 0:
            table_copy.wait()
            table = (table_ref[0], table_ref[1])
        for pair in range(LOC // 2):
            value = jnp.concatenate(
                [field[half, pl.ds(2 * pair + k, N, stride=LOC), :] for k in range(2)], axis=1
            )
            value = dot3(table, split(value))
            if half == 0:
                partial[pair] = value
            else:
                real = partial[pair, :N] - value[N:]
                imag = partial[pair, N:] + value[:N]
                for k in range(2):
                    lanes = slice(k * ZM, (k + 1) * ZM)
                    out[:, 0, 2 * pair + k] = real[:, lanes].reshape(GRID, LOC, ZM)
                    out[:, 1, 2 * pair + k] = imag[:, lanes].reshape(GRID, LOC, ZM)
                rows = pl.ds(2 * pair, 2)
                sent.append(pltpu.make_async_copy(out.at[:, :, rows], out_hbm.at[:, :, rows], sems.at[4, pair]))
                sent[-1].start()
    for copy in sent:
        copy.wait()


def plane_kernel(
    rank_ref, in_ref, noise_hbm, tables_hbm, out_ref, base, noise_ref, tables, sems
):
    step = pl.program_id(0)
    groups = LOC // STEP_PLANES
    table_copies = [
        pltpu.make_async_copy(tables_hbm.at[part], tables.at[part], sems.at[groups + k])
        for k, part in enumerate((pl.ds(0, 2), pl.ds(2, 2), pl.ds(4, 4)))
    ]

    def noise_copy(group):
        planes = pl.ds(group * STEP_PLANES, STEP_PLANES)
        return pltpu.make_async_copy(noise_hbm.at[0, :, planes], noise_ref.at[:, planes], sems.at[group])

    def to_field(group):
        lanes = []
        for inner in range(STEP_PLANES):
            rows = pl.ds(group * STEP_PLANES + inner, LOC, stride=LOC)
            real = jnp.concatenate([in_ref[g, 0, rows, :] for g in range(GRID)], axis=0)
            imag = jnp.concatenate([in_ref[g, 1, rows, :] for g in range(GRID)], axis=0)
            real, imag = column_transform((tables[0], tables[1]), real, imag)
            lanes.append(jnp.concatenate([real, imag], axis=1))
        value = split(jnp.concatenate(lanes, axis=0))
        parts = (pl.ds(0, N), pl.ds(N, N))
        return [dot3(value, (tables[2, lines], tables[3, lines])) for lines in parts]

    def from_field(group, field):
        lanes = []
        for inner in range(STEP_PLANES):
            plane = group * STEP_PLANES + inner
            pos_x = ((rank_ref[0] * LOC + plane).astype(F32) + 0.5) / N - 0.5
            shift_x = (TURN * trap_strength) * pos_x * pos_x
            real = field[0][inner * N : (inner + 1) * N]
            imag = field[1][inner * N : (inner + 1) * N]
            turns = (base[...] + shift_x) + (TURN * coupling) * (real * real + imag * imag)
            rest = turns - jnp.round(turns)
            square = rest * rest
            sine = polynomial(SIN_C, square) * rest
            cosine = polynomial(COS_C, square)
            decay = jnp.exp2(turns * DECAY_LOG2 + AMP_LOG2)
            evo_real = decay * (1.0 - sine * sine)
            evo_imag = decay * (sine * cosine)
            moved_real = real * evo_real + imag * evo_imag + noise_ref[0, plane]
            moved_imag = imag * evo_real - real * evo_imag + noise_ref[1, plane]
            lanes.append(jnp.concatenate([moved_real, moved_imag], axis=1))
        value = dot3(split(jnp.concatenate(lanes, axis=0)), (tables[4], tables[5]))
        for inner in range(STEP_PLANES):
            rows = pl.ds(group * STEP_PLANES + inner, LOC, stride=LOC)
            both = value[inner * N : (inner + 1) * N]
            real, imag = column_transform((tables[6], tables[7]), both[:, :ZM], both[:, ZM:])
            for g in range(GRID):
                out_ref[g, 0, rows, :] = real[g * LOC : (g + 1) * LOC]
                out_ref[g, 1, rows, :] = imag[g * LOC : (g + 1) * LOC]

    @pl.when(step == 0)
    def _():
        table_copies[0].start()
        table_copies[1].start()
        shape = (N, N)
        pos_y = (lax.broadcasted_iota(jnp.int32, shape, 0).astype(F32) + 0.5) / N - 0.5
        pos_z = (lax.broadcasted_iota(jnp.int32, shape, 1).astype(F32) + 0.5) / N - 0.5
        base[...] = TURN * (trap_strength * (pos_y * pos_y + pos_z * pos_z) - chem_potential)
        table_copies[0].wait()
        noise_copy(0).start()
        table_copies[2].start()
        table_copies[1].wait()
        for later in range(1, groups):
            noise_copy(later).start()

    field = to_field(step)
    noise_copy(step).wait()

    @pl.when(step == 0)
    def _():
        table_copies[2].wait()

    from_field(step, field)


def last_kernel(
    rank_ref, in_ref, mask_ref, table_ref, out_hbm, hist_ref, keep, field, occ, halves_ref, sems
):
    keep[...] = select_tiles(mask_ref[...]).astype(F32).reshape(N * LOC, ZM)
    lines = field.reshape(2, 2, N * LOC, ZM)
    half_rows = N // 2
    low_lane = lax.broadcasted_iota(jnp.int32, (half_rows, ZM), 1) < ZM // 2
    far = jnp.zeros((8, ZM), F32)
    mirror = lax.broadcasted_iota(jnp.int32, (NEAR, ZM), 1)
    low_near = mirror < ZM // 2
    mirror = jnp.where((mirror & (ZM // 2 - 1)) == 0, ZM // 2 - mirror, ZM - mirror)
    copies = []
    for upper in range(2):
        first = upper * half_rows
        table = tuple(
            jnp.concatenate(
                [table_ref[k, first : first + half_rows], table_ref[k, N + first : N + first + half_rows]], axis=0
            )
            for k in range(2)
        )
        even = None
        for row in range(LOC):
            if upper == 0:
                value = jnp.concatenate(
                    [in_ref[:, 0, row].reshape(N, ZM), in_ref[:, 1, row].reshape(N, ZM)], axis=1
                )
                held = split(value)
                halves_ref[row, 0] = held[0]
                halves_ref[row, 1] = held[1]
            else:
                held = halves_ref[row, 0], halves_ref[row, 1]
            both = dot3(table, held)
            real = both[:half_rows, :ZM] - both[half_rows:, ZM:]
            imag = both[:half_rows, ZM:] + both[half_rows:, :ZM]
            rows = pl.ds(first * LOC + row, half_rows, stride=LOC)
            mask = keep[rows, :]
            real = real * mask
            imag = imag * mask
            for half, value in enumerate((real, imag)):
                lines[half, 0, rows, :] = jnp.where(low_lane, value, 0.0)
                lines[half, 1, rows, :] = jnp.where(low_lane, 0.0, value)
            occupation = real * real + imag * imag
            if upper == 0:
                near, rest = occupation[:NEAR], occupation[NEAR:]
            else:
                rest, near = occupation[: half_rows - NEAR], occupation[half_rows - NEAR :]
            far = far + jnp.sum(rest.reshape(-1, 8, ZM), axis=0)
            if row % 2 == 0:
                even = near
                continue
            folded = jnp.where(low_near, even, near) + jnp.take_along_axis(
                jnp.where(low_near, near, even), mirror, axis=1, mode="promise_in_bounds"
            )
            high, low = split(folded)
            lanes = slice(row // 2 * ZM, (row // 2 + 1) * ZM)
            occ[upper * NEAR : (upper + 1) * NEAR, lanes] = high
            occ[(2 + upper) * NEAR : (3 + upper) * NEAR, lanes] = low
        part = pl.ds(first, half_rows)
        for half in range(2):
            for tile in range(2):
                copies.append(
                    pltpu.make_async_copy(
                        field.at[half, tile, part],
                        out_hbm.at[0, half, part, :, pl.ds(tile * ZM, ZM)],
                        sems.at[half, 2 * upper + tile],
                    )
                )
                copies[-1].start()

    shape = (LOC * ZM // 2, SHELLS)
    place = lax.broadcasted_iota(jnp.int32, shape, 0)
    lane = place & (ZM - 1)
    index_y = rank_ref[0] * LOC + 2 * (place >> 7) + (lane >> 6)
    sig_y = jnp.where(index_y < N // 2, index_y, index_y - N)
    sig_z = jnp.where(lane < ZM // 2, lane, (ZM - lane) & (ZM // 2 - 1))
    rest = jnp.minimum(sig_y * sig_y + sig_z * sig_z, 64 * (SHELLS - 1))
    gap = (rest - 64 * lax.broadcasted_iota(jnp.int32, shape, 1)).astype(F32)
    gap = jnp.clip(gap, -GAP_MAX, GAP_MAX).astype(BF16)
    count = 2 * NEAR
    shape = (count, SHELLS)
    index_x = lax.broadcasted_iota(jnp.int32, shape, 0)
    sig_x = jnp.where(index_x < NEAR, index_x, index_x - count)
    square_x = sig_x * sig_x
    residue = square_x & 63
    sums = jnp.zeros(shape, F32)
    one = jnp.ones((), BF16)
    zero = jnp.zeros((), BF16)
    for first in range(0, len(RESIDUES), 2):
        pair = RESIDUES[first : first + 2]
        hits = jnp.concatenate(
            [jnp.where(jnp.abs(gap + BF16(r - 31.5)) < BF16(32.0), one, zero) for r in pair], axis=1
        )
        found = dot(occ[...], hits)
        found = found[:count] + found[count:]
        for place_of, r in enumerate(pair):
            sums = jnp.where(residue == r, found[:, place_of * SHELLS : (place_of + 1) * SHELLS], sums)
    moves = square_x >> 6
    bins = lax.broadcasted_iota(jnp.int32, shape, 1)
    beyond = moves >= SHELLS - 1
    over = jnp.where(beyond, sums, 0.0)
    sums = jnp.where(beyond, 0.0, sums)
    for bit in range(7):
        width = 1 << bit
        chosen = (moves & width) != 0
        past = chosen & (bins >= SHELLS - width)
        over = over + jnp.where(past, sums, 0.0)
        rolled = jnp.where(bins >= width, pltpu.roll(sums, width, 1), 0.0)
        sums = jnp.where(chosen, rolled, sums)
    total = jnp.sum(sums, axis=0, keepdims=True)
    extra = jnp.sum(over, axis=0, keepdims=True) + jnp.sum(far, axis=0, keepdims=True)
    extra = jnp.sum(extra, axis=1, keepdims=True)
    hist = total + jnp.where(bins[:1] == SHELLS - 1, extra, 0.0)
    hist_ref[...] = jnp.broadcast_to(hist.reshape(1, 1, SHELLS), (GRID, 1, SHELLS))
    for copy in copies:
        copy.wait()


def params(mib):
    return pltpu.CompilerParams(vmem_limit_bytes=mib * 1024 * 1024)


def whole(shape):
    return pl.BlockSpec(shape, lambda *_: (0,) * len(shape))


def exchange(value):
    return lax.all_to_all(value, "grid", split_axis=0, concat_axis=0, tiled=True)


def shards(psi_modes, noise, mask):
    inv_tall, fwd_tall, inv_z, fwd_z = (halves(table) for table in host_tables())
    tables = jnp.asarray(np.concatenate([inv_tall, inv_z, fwd_z, fwd_tall]))
    rank = lax.axis_index("grid").astype(jnp.int32).reshape(1)
    smem = pl.BlockSpec(memory_space=pltpu.SMEM)
    hbm = pl.BlockSpec(memory_space=pltpu.HBM)
    message = (GRID, 2, LOC, LOC, ZM)
    flat = (GRID, 2, LOC * LOC, ZM)
    sent = pl.pallas_call(
        first_kernel,
        out_shape=jax.ShapeDtypeStruct(message, F32),
        grid=(1,),
        in_specs=[hbm] * 3,
        out_specs=hbm,
        scratch_shapes=[
            pltpu.VMEM((2, N, LOC, N), F32),
            pltpu.VMEM((N, LOC, N), jnp.int32),
            pltpu.VMEM((2, 2 * N, N), BF16),
            pltpu.VMEM((N * LOC, ZM), F32),
            pltpu.VMEM((2, N * LOC, ZM), F32),
            pltpu.VMEM((LOC // 2, 2 * N, 2 * ZM), F32),
            pltpu.VMEM(message, F32),
            pltpu.SemaphoreType.DMA((5, 4)),
        ],
        compiler_params=params(63),
        name="first",
    )(psi_modes, mask, tables)
    planes = exchange(sent).reshape(flat)
    sent = pl.pallas_call(
        plane_kernel,
        out_shape=jax.ShapeDtypeStruct(flat, F32),
        grid=(LOC // STEP_PLANES,),
        in_specs=[
            smem,
            whole(flat),
            hbm,
            hbm,
        ],
        out_specs=whole(flat),
        scratch_shapes=[
            pltpu.VMEM((N, N), F32),
            pltpu.VMEM((2, LOC, N, N), F32),
            pltpu.VMEM(tables.shape, BF16),
            pltpu.SemaphoreType.DMA((LOC // STEP_PLANES + 3,)),
        ],
        compiler_params=params(PLANES_MIB),
        name="planes",
    )(rank, planes, noise, tables)
    rows_in = exchange(sent).reshape(message)
    psi_next, hist = pl.pallas_call(
        last_kernel,
        out_shape=(
            jax.ShapeDtypeStruct(psi_modes.shape, F32),
            jax.ShapeDtypeStruct((GRID, 1, SHELLS), F32),
        ),
        grid=(1,),
        in_specs=[smem, whole(message), whole((N, LOC, N)), pl.BlockSpec((2, 2 * N, N), lambda i: (3, 0, 0))],
        out_specs=(hbm, whole((GRID, 1, SHELLS))),
        scratch_shapes=[
            pltpu.VMEM((N * LOC, ZM), F32),
            pltpu.VMEM((2, 2, N, LOC, ZM), F32),
            pltpu.VMEM((4 * NEAR, LOC * ZM // 2), BF16),
            pltpu.VMEM((LOC, 2, N, 2 * ZM), BF16),
            pltpu.SemaphoreType.DMA((2, 4)),
        ],
        compiler_params=params(24),
        name="last",
    )(rank, rows_in, mask, tables)
    hist = jnp.sum(exchange(hist), axis=0)
    other = [lax.ppermute(hist, "traj", [(t, (t + k) % TRAJ) for t in range(TRAJ)]) for k in (1, 2, 3)]
    hist = (hist + other[1]) + (other[0] + other[2])
    return psi_next, hist.reshape(SHELLS) * (SHELLS / (TRAJ * N * N * N))


def solution(mesh):
    placed = (
        P("traj", None, None, "grid", None),
        P("traj", None, "grid", None, None),
        P(None, "grid", None),
    )
    return jax.shard_map(
        shards,
        mesh=mesh,
        in_specs=placed,
        out_specs=(P("traj", None, None, "grid", None), P()),
        check_vma=False,
    )
```

```python
import jax
import jax.numpy as jnp
import numpy as np
from jax import lax
from jax.experimental import pallas as pl
from jax.experimental.pallas import tpu as pltpu
from jax.sharding import PartitionSpec as P

SHELLS = 128
N = 256
GRID = 32
LOC = N // GRID
ZM = N // 2
TRAJ = 4
PLANES_MIB = 48
STEP_PLANES = 8

time_step = 1.0
damping = 0.05
coupling = 10.0
chem_potential = 1.0
noise_amp = 0.1
trap_strength = 8.0

F32 = jnp.float32
BF16 = jnp.bfloat16

RESIDUES = sorted({(s * s) % 64 for s in range(64)})
NEAR = 96
GAP_MAX = 100.0

SIN_C = [
    c * np.sqrt(2.0) * np.pi ** (2 * k + 1)
    for k, c in enumerate((0.9999999957052124, -0.1666665795268036, 0.008333050198586583, -0.00019809014686181177, 2.6050929465880504e-06))
]
COS_C = [
    c * np.sqrt(2.0) * np.pi ** (2 * k)
    for k, c in enumerate((0.9999999531318189, -0.49999904875147083, 0.041663574368409804, -0.0013853632426514488, 2.3152375214584864e-05))
]
TURN = time_step / (2.0 * np.pi)
DECAY_LOG2 = -damping * 2.0 * np.pi / np.log(2.0)
AMP_LOG2 = -np.log2(noise_amp)


def host_tables():
    index = np.arange(N)
    signed = np.where(index < N // 2, index, index - N)
    wave = signed * (2.0 * np.pi / N)
    step = np.exp(-(damping + 1j) * 0.25 * time_step * wave**2)
    phase = np.exp(2j * np.pi * ((index[:, None] * index[None, :]) % N) / N) / np.sqrt(N)
    inverse = phase * step[None, :]
    forward = np.conj(phase) * step[:, None]
    cols = np.concatenate([index[: N // 4], index[3 * N // 4 :]])
    inv_tall = np.concatenate([inverse.real, inverse.imag], 0)
    fwd_tall = np.concatenate([forward.real, forward.imag], 0)
    iz = inverse[:, cols].T
    inv_z = np.concatenate([iz.real, -iz.imag, iz.imag, iz.real], 0)
    fz = noise_amp * forward[cols, :].T
    fwd_z = np.block([[fz.real, fz.imag], [-fz.imag, fz.real]])
    return inv_tall, fwd_tall, inv_z, fwd_z


def halves(table):
    table = np.asarray(table, np.float32)
    high = table.astype(BF16)
    low = (table - high.astype(np.float32)).astype(BF16)
    return np.stack([high, low])


def split(value):
    high = value.astype(BF16)
    return high, (value - high.astype(F32)).astype(BF16)


def dot(left, right):
    return jnp.dot(left, right, preferred_element_type=F32)


def dot3(left, right):
    return dot(left[0], right[0]) + dot(left[0], right[1]) + dot(left[1], right[0])


def column_transform(table, real, imag):
    count = real.shape[1]
    both = dot3(table, split(jnp.concatenate([real, imag], axis=1)))
    top, low = both[:N], both[N:]
    return top[:, :count] - low[:, count:], top[:, count:] + low[:, :count]


def select_tiles(values):
    lane = lax.broadcasted_iota(jnp.int32, values.shape[:-1] + (ZM,), values.ndim - 1)
    return jnp.where(lane < ZM // 2, values[..., :ZM], values[..., ZM:])


def polynomial(coefs, square):
    value = coefs[-1]
    for coef in coefs[-2::-1]:
        value = value * square + coef
    return value


def first_kernel(psi_hbm, mask_hbm, table_hbm, out_hbm, psi, mask, table_ref, keep, field, partial, out, sems):
    pieces = 4
    count = N // pieces
    copies = [[], [], []]
    for piece in range(pieces):
        part = pl.ds(piece * count, count)
        copies[0].append(pltpu.make_async_copy(mask_hbm.at[part], mask.at[part], sems.at[0, piece]))
        for half in range(2):
            copies[1 + half].append(
                pltpu.make_async_copy(psi_hbm.at[0, half, part], psi.at[half, part], sems.at[1 + half, piece])
            )
    table_copy = pltpu.make_async_copy(table_hbm.at[pl.ds(0, 2)], table_ref, sems.at[3, 0])
    for pair in zip(*copies[:2]):
        for copy in pair:
            copy.start()
    table_copy.start()
    table = None
    sent = []
    for half in range(2):
        for piece in range(pieces):
            part = slice(piece * count, (piece + 1) * count)
            lines = slice(piece * count * LOC, (piece + 1) * count * LOC)
            if half == 0:
                copies[0][piece].wait()
                keep[lines] = select_tiles(mask[part]).astype(F32).reshape(count * LOC, ZM)
            copies[1 + half][piece].wait()
            if half == 0:
                copies[2][piece].start()
            field[half, lines] = select_tiles(psi[half, part]).reshape(count * LOC, ZM) * keep[lines]
        if half == 0:
            table_copy.wait()
            table = (table_ref[0], table_ref[1])
        for pair in range(LOC // 2):
            value = jnp.concatenate(
                [field[half, pl.ds(2 * pair + k, N, stride=LOC), :] for k in range(2)], axis=1
            )
            value = dot3(table, split(value))
            if half == 0:
                partial[pair] = value
            else:
                real = partial[pair, :N] - value[N:]
                imag = partial[pair, N:] + value[:N]
                for k in range(2):
                    lanes = slice(k * ZM, (k + 1) * ZM)
                    out[:, 0, 2 * pair + k] = real[:, lanes].reshape(GRID, LOC, ZM)
                    out[:, 1, 2 * pair + k] = imag[:, lanes].reshape(GRID, LOC, ZM)
                rows = pl.ds(2 * pair, 2)
                sent.append(pltpu.make_async_copy(out.at[:, :, rows], out_hbm.at[:, :, rows], sems.at[4, pair]))
                sent[-1].start()
    for copy in sent:
        copy.wait()


def plane_kernel(
    rank_ref, in_ref, noise_hbm, tables_hbm, out_ref, base, noise_ref, tables, sems
):
    step = pl.program_id(0)
    groups = LOC // STEP_PLANES
    table_copies = [
        pltpu.make_async_copy(tables_hbm.at[part], tables.at[part], sems.at[groups + k])
        for k, part in enumerate((pl.ds(0, 2), pl.ds(2, 2), pl.ds(4, 4)))
    ]

    def noise_copy(group):
        planes = pl.ds(group * STEP_PLANES, STEP_PLANES)
        return pltpu.make_async_copy(noise_hbm.at[0, :, planes], noise_ref.at[:, planes], sems.at[group])

    def to_field(group):
        lanes = []
        for inner in range(STEP_PLANES):
            rows = pl.ds(group * STEP_PLANES + inner, LOC, stride=LOC)
            real = jnp.concatenate([in_ref[g, 0, rows, :] for g in range(GRID)], axis=0)
            imag = jnp.concatenate([in_ref[g, 1, rows, :] for g in range(GRID)], axis=0)
            real, imag = column_transform((tables[0], tables[1]), real, imag)
            lanes.append(jnp.concatenate([real, imag], axis=1))
        value = split(jnp.concatenate(lanes, axis=0))
        parts = (pl.ds(0, N), pl.ds(N, N))
        return [dot3(value, (tables[2, lines], tables[3, lines])) for lines in parts]

    def from_field(group, field):
        lanes = []
        for inner in range(STEP_PLANES):
            plane = group * STEP_PLANES + inner
            pos_x = ((rank_ref[0] * LOC + plane).astype(F32) + 0.5) / N - 0.5
            shift_x = (TURN * trap_strength) * pos_x * pos_x
            real = field[0][inner * N : (inner + 1) * N]
            imag = field[1][inner * N : (inner + 1) * N]
            turns = (base[...] + shift_x) + (TURN * coupling) * (real * real + imag * imag)
            rest = turns - jnp.round(turns)
            square = rest * rest
            sine = polynomial(SIN_C, square) * rest
            cosine = polynomial(COS_C, square)
            decay = jnp.exp2(turns * DECAY_LOG2 + AMP_LOG2)
            evo_real = decay * (1.0 - sine * sine)
            evo_imag = decay * (sine * cosine)
            moved_real = real * evo_real + imag * evo_imag + noise_ref[0, plane]
            moved_imag = imag * evo_real - real * evo_imag + noise_ref[1, plane]
            lanes.append(jnp.concatenate([moved_real, moved_imag], axis=1))
        value = dot3(split(jnp.concatenate(lanes, axis=0)), (tables[4], tables[5]))
        for inner in range(STEP_PLANES):
            rows = pl.ds(group * STEP_PLANES + inner, LOC, stride=LOC)
            both = value[inner * N : (inner + 1) * N]
            real, imag = column_transform((tables[6], tables[7]), both[:, :ZM], both[:, ZM:])
            for g in range(GRID):
                out_ref[g, 0, rows, :] = real[g * LOC : (g + 1) * LOC]
                out_ref[g, 1, rows, :] = imag[g * LOC : (g + 1) * LOC]

    @pl.when(step == 0)
    def _():
        table_copies[0].start()
        table_copies[1].start()
        shape = (N, N)
        pos_y = (lax.broadcasted_iota(jnp.int32, shape, 0).astype(F32) + 0.5) / N - 0.5
        pos_z = (lax.broadcasted_iota(jnp.int32, shape, 1).astype(F32) + 0.5) / N - 0.5
        base[...] = TURN * (trap_strength * (pos_y * pos_y + pos_z * pos_z) - chem_potential)
        table_copies[0].wait()
        noise_copy(0).start()
        table_copies[2].start()
        table_copies[1].wait()
        for later in range(1, groups):
            noise_copy(later).start()

    field = to_field(step)
    noise_copy(step).wait()

    @pl.when(step == 0)
    def _():
        table_copies[2].wait()

    from_field(step, field)


def last_kernel(
    rank_ref, in_ref, mask_ref, table_ref, out_hbm, hist_ref, keep, field, occ, halves_ref, sems
):
    keep[...] = select_tiles(mask_ref[...]).astype(F32).reshape(N * LOC, ZM)
    lines = field.reshape(2, 2, N * LOC, ZM)
    half_rows = N // 2
    low_lane = lax.broadcasted_iota(jnp.int32, (half_rows, ZM), 1) < ZM // 2
    far = jnp.zeros((8, ZM), F32)
    mirror = lax.broadcasted_iota(jnp.int32, (NEAR, ZM), 1)
    low_near = mirror < ZM // 2
    mirror = jnp.where((mirror & (ZM // 2 - 1)) == 0, ZM // 2 - mirror, ZM - mirror)
    copies = []
    for upper in range(2):
        first = upper * half_rows
        table = tuple(
            jnp.concatenate(
                [table_ref[k, first : first + half_rows], table_ref[k, N + first : N + first + half_rows]], axis=0
            )
            for k in range(2)
        )
        even = None
        for row in range(LOC):
            if upper == 0:
                value = jnp.concatenate(
                    [in_ref[:, 0, row].reshape(N, ZM), in_ref[:, 1, row].reshape(N, ZM)], axis=1
                )
                held = split(value)
                halves_ref[row, 0] = held[0]
                halves_ref[row, 1] = held[1]
            else:
                held = halves_ref[row, 0], halves_ref[row, 1]
            both = dot3(table, held)
            real = both[:half_rows, :ZM] - both[half_rows:, ZM:]
            imag = both[:half_rows, ZM:] + both[half_rows:, :ZM]
            rows = pl.ds(first * LOC + row, half_rows, stride=LOC)
            mask = keep[rows, :]
            real = real * mask
            imag = imag * mask
            for half, value in enumerate((real, imag)):
                lines[half, 0, rows, :] = jnp.where(low_lane, value, 0.0)
                lines[half, 1, rows, :] = jnp.where(low_lane, 0.0, value)
            occupation = real * real + imag * imag
            if upper == 0:
                near, rest = occupation[:NEAR], occupation[NEAR:]
            else:
                rest, near = occupation[: half_rows - NEAR], occupation[half_rows - NEAR :]
            far = far + jnp.sum(rest.reshape(-1, 8, ZM), axis=0)
            if row % 2 == 0:
                even = near
                continue
            folded = jnp.where(low_near, even, near) + jnp.take_along_axis(
                jnp.where(low_near, near, even), mirror, axis=1, mode="promise_in_bounds"
            )
            high, low = split(folded)
            lanes = slice(row // 2 * ZM, (row // 2 + 1) * ZM)
            occ[upper * NEAR : (upper + 1) * NEAR, lanes] = high
            occ[(2 + upper) * NEAR : (3 + upper) * NEAR, lanes] = low
        part = pl.ds(first, half_rows)
        for half in range(2):
            for tile in range(2):
                copies.append(
                    pltpu.make_async_copy(
                        field.at[half, tile, part],
                        out_hbm.at[0, half, part, :, pl.ds(tile * ZM, ZM)],
                        sems.at[half, 2 * upper + tile],
                    )
                )
                copies[-1].start()

    shape = (LOC * ZM // 2, SHELLS)
    place = lax.broadcasted_iota(jnp.int32, shape, 0)
    lane = place & (ZM - 1)
    index_y = rank_ref[0] * LOC + 2 * (place >> 7) + (lane >> 6)
    sig_y = jnp.where(index_y < N // 2, index_y, index_y - N)
    sig_z = jnp.where(lane < ZM // 2, lane, (ZM - lane) & (ZM // 2 - 1))
    rest = jnp.minimum(sig_y * sig_y + sig_z * sig_z, 64 * (SHELLS - 1))
    gap = (rest - 64 * lax.broadcasted_iota(jnp.int32, shape, 1)).astype(F32)
    gap = jnp.clip(gap, -GAP_MAX, GAP_MAX).astype(BF16)
    count = 2 * NEAR
    shape = (count, SHELLS)
    index_x = lax.broadcasted_iota(jnp.int32, shape, 0)
    sig_x = jnp.where(index_x < NEAR, index_x, index_x - count)
    square_x = sig_x * sig_x
    residue = square_x & 63
    sums = jnp.zeros(shape, F32)
    one = jnp.ones((), BF16)
    zero = jnp.zeros((), BF16)
    for first in range(0, len(RESIDUES), 2):
        pair = RESIDUES[first : first + 2]
        hits = jnp.concatenate(
            [jnp.where(jnp.abs(gap + BF16(r - 31.5)) < BF16(32.0), one, zero) for r in pair], axis=1
        )
        found = dot(occ[...], hits)
        found = found[:count] + found[count:]
        for place_of, r in enumerate(pair):
            sums = jnp.where(residue == r, found[:, place_of * SHELLS : (place_of + 1) * SHELLS], sums)
    moves = square_x >> 6
    bins = lax.broadcasted_iota(jnp.int32, shape, 1)
    beyond = moves >= SHELLS - 1
    over = jnp.where(beyond, sums, 0.0)
    sums = jnp.where(beyond, 0.0, sums)
    for bit in range(7):
        width = 1 << bit
        chosen = (moves & width) != 0
        past = chosen & (bins >= SHELLS - width)
        over = over + jnp.where(past, sums, 0.0)
        rolled = jnp.where(bins >= width, pltpu.roll(sums, width, 1), 0.0)
        sums = jnp.where(chosen, rolled, sums)
    total = jnp.sum(sums, axis=0, keepdims=True)
    extra = jnp.sum(over, axis=0, keepdims=True) + jnp.sum(far, axis=0, keepdims=True)
    extra = jnp.sum(extra, axis=1, keepdims=True)
    hist = total + jnp.where(bins[:1] == SHELLS - 1, extra, 0.0)
    hist_ref[...] = jnp.broadcast_to(hist.reshape(1, 1, SHELLS), (GRID, 1, SHELLS))
    for copy in copies:
        copy.wait()


def params(mib):
    return pltpu.CompilerParams(vmem_limit_bytes=mib * 1024 * 1024)


def whole(shape):
    return pl.BlockSpec(shape, lambda *_: (0,) * len(shape))


def exchange(value):
    return lax.all_to_all(value, "grid", split_axis=0, concat_axis=0, tiled=True)


def shards(psi_modes, noise, mask):
    inv_tall, fwd_tall, inv_z, fwd_z = (halves(table) for table in host_tables())
    tables = jnp.asarray(np.concatenate([inv_tall, inv_z, fwd_z, fwd_tall]))
    rank = lax.axis_index("grid").astype(jnp.int32).reshape(1)
    smem = pl.BlockSpec(memory_space=pltpu.SMEM)
    hbm = pl.BlockSpec(memory_space=pltpu.HBM)
    message = (GRID, 2, LOC, LOC, ZM)
    flat = (GRID, 2, LOC * LOC, ZM)
    sent = pl.pallas_call(
        first_kernel,
        out_shape=jax.ShapeDtypeStruct(message, F32),
        grid=(1,),
        in_specs=[hbm] * 3,
        out_specs=hbm,
        scratch_shapes=[
            pltpu.VMEM((2, N, LOC, N), F32),
            pltpu.VMEM((N, LOC, N), jnp.int32),
            pltpu.VMEM((2, 2 * N, N), BF16),
            pltpu.VMEM((N * LOC, ZM), F32),
            pltpu.VMEM((2, N * LOC, ZM), F32),
            pltpu.VMEM((LOC // 2, 2 * N, 2 * ZM), F32),
            pltpu.VMEM(message, F32),
            pltpu.SemaphoreType.DMA((5, 4)),
        ],
        compiler_params=params(63),
        name="first",
    )(psi_modes, mask, tables)
    planes = exchange(sent).reshape(flat)
    sent = pl.pallas_call(
        plane_kernel,
        out_shape=jax.ShapeDtypeStruct(flat, F32),
        grid=(LOC // STEP_PLANES,),
        in_specs=[
            smem,
            whole(flat),
            hbm,
            hbm,
        ],
        out_specs=whole(flat),
        scratch_shapes=[
            pltpu.VMEM((N, N), F32),
            pltpu.VMEM((2, LOC, N, N), F32),
            pltpu.VMEM(tables.shape, BF16),
            pltpu.SemaphoreType.DMA((LOC // STEP_PLANES + 3,)),
        ],
        compiler_params=params(PLANES_MIB),
        name="planes",
    )(rank, planes, noise, tables)
    rows_in = exchange(sent).reshape(message)
    psi_next, hist = pl.pallas_call(
        last_kernel,
        out_shape=(
            jax.ShapeDtypeStruct(psi_modes.shape, F32),
            jax.ShapeDtypeStruct((GRID, 1, SHELLS), F32),
        ),
        grid=(1,),
        in_specs=[smem, whole(message), whole((N, LOC, N)), pl.BlockSpec((2, 2 * N, N), lambda i: (3, 0, 0))],
        out_specs=(hbm, whole((GRID, 1, SHELLS))),
        scratch_shapes=[
            pltpu.VMEM((N * LOC, ZM), F32),
            pltpu.VMEM((2, 2, N, LOC, ZM), F32),
            pltpu.VMEM((4 * NEAR, LOC * ZM // 2), BF16),
            pltpu.VMEM((LOC, 2, N, 2 * ZM), BF16),
            pltpu.SemaphoreType.DMA((2, 4)),
        ],
        compiler_params=params(24),
        name="last",
    )(rank, rows_in, mask, tables)
    hist = jnp.sum(exchange(hist), axis=0)
    other = [lax.ppermute(hist, "traj", [(t, (t + k) % TRAJ) for t in range(TRAJ)]) for k in (1, 2, 3)]
    hist = (hist + other[1]) + (other[0] + other[2])
    return psi_next, hist.reshape(SHELLS) * (SHELLS / (TRAJ * N * N * N))


def solution(mesh):
    placed = (
        P("traj", None, None, "grid", None),
        P("traj", None, "grid", None, None),
        P(None, "grid", None),
    )
    return jax.shard_map(
        shards,
        mesh=mesh,
        in_specs=placed,
        out_specs=(P("traj", None, None, "grid", None), P()),
        check_vma=False,
    )
```

```python
import jax
import jax.numpy as jnp
import numpy as np
from jax import lax
from jax.experimental import pallas as pl
from jax.experimental.pallas import tpu as pltpu
from jax.sharding import PartitionSpec as P

SHELLS = 128
N = 256
GRID = 32
LOC = N // GRID
ZM = N // 2
TRAJ = 4
PLANES_MIB = 48
STEP_PLANES = 8

time_step = 1.0
damping = 0.05
coupling = 10.0
chem_potential = 1.0
noise_amp = 0.1
trap_strength = 8.0

F32 = jnp.float32
BF16 = jnp.bfloat16

RESIDUES = sorted({(s * s) % 64 for s in range(64)})
NEAR = 96
GAP_MAX = 100.0

SIN_C = [
    c * np.sqrt(2.0) * np.pi ** (2 * k + 1)
    for k, c in enumerate((0.9999999957052124, -0.1666665795268036, 0.008333050198586583, -0.00019809014686181177, 2.6050929465880504e-06))
]
COS_C = [
    c * np.sqrt(2.0) * np.pi ** (2 * k)
    for k, c in enumerate((0.9999999531318189, -0.49999904875147083, 0.041663574368409804, -0.0013853632426514488, 2.3152375214584864e-05))
]
TURN = time_step / (2.0 * np.pi)
DECAY_LOG2 = -damping * 2.0 * np.pi / np.log(2.0)
AMP_LOG2 = -np.log2(noise_amp)


def host_tables():
    index = np.arange(N)
    signed = np.where(index < N // 2, index, index - N)
    wave = signed * (2.0 * np.pi / N)
    step = np.exp(-(damping + 1j) * 0.25 * time_step * wave**2)
    phase = np.exp(2j * np.pi * ((index[:, None] * index[None, :]) % N) / N) / np.sqrt(N)
    inverse = phase * step[None, :]
    forward = np.conj(phase) * step[:, None]
    cols = np.concatenate([index[: N // 4], index[3 * N // 4 :]])
    inv_tall = np.concatenate([inverse.real, inverse.imag], 0)
    fwd_tall = np.concatenate([forward.real, forward.imag], 0)
    iz = inverse[:, cols].T
    inv_z = np.concatenate([iz.real, -iz.imag, iz.imag, iz.real], 0)
    fz = noise_amp * forward[cols, :].T
    fwd_z = np.block([[fz.real, fz.imag], [-fz.imag, fz.real]])
    return inv_tall, fwd_tall, inv_z, fwd_z


def halves(table):
    table = np.asarray(table, np.float32)
    high = table.astype(BF16)
    low = (table - high.astype(np.float32)).astype(BF16)
    return np.stack([high, low])


def split(value):
    high = value.astype(BF16)
    return high, (value - high.astype(F32)).astype(BF16)


def dot(left, right):
    return jnp.dot(left, right, preferred_element_type=F32)


def dot3(left, right):
    return dot(left[0], right[0]) + dot(left[0], right[1]) + dot(left[1], right[0])


def column_transform(table, real, imag):
    count = real.shape[1]
    both = dot3(table, split(jnp.concatenate([real, imag], axis=1)))
    top, low = both[:N], both[N:]
    return top[:, :count] - low[:, count:], top[:, count:] + low[:, :count]


def select_tiles(values):
    lane = lax.broadcasted_iota(jnp.int32, values.shape[:-1] + (ZM,), values.ndim - 1)
    return jnp.where(lane < ZM // 2, values[..., :ZM], values[..., ZM:])


def polynomial(coefs, square):
    value = coefs[-1]
    for coef in coefs[-2::-1]:
        value = value * square + coef
    return value


def first_kernel(psi_hbm, mask_hbm, table_hbm, out_hbm, psi, mask, table_ref, keep, field, partial, out, sems):
    pieces = 4
    count = N // pieces
    copies = [[], [], []]
    for piece in range(pieces):
        part = pl.ds(piece * count, count)
        copies[0].append(pltpu.make_async_copy(mask_hbm.at[part], mask.at[part], sems.at[0, piece]))
        for half in range(2):
            copies[1 + half].append(
                pltpu.make_async_copy(psi_hbm.at[0, half, part], psi.at[half, part], sems.at[1 + half, piece])
            )
    table_copy = pltpu.make_async_copy(table_hbm.at[pl.ds(0, 2)], table_ref, sems.at[3, 0])
    for pair in zip(*copies[:2]):
        for copy in pair:
            copy.start()
    table_copy.start()
    table = None
    sent = []
    for half in range(2):
        for piece in range(pieces):
            part = slice(piece * count, (piece + 1) * count)
            lines = slice(piece * count * LOC, (piece + 1) * count * LOC)
            if half == 0:
                copies[0][piece].wait()
                keep[lines] = select_tiles(mask[part]).astype(F32).reshape(count * LOC, ZM)
            copies[1 + half][piece].wait()
            if half == 0:
                copies[2][piece].start()
            field[half, lines] = select_tiles(psi[half, part]).reshape(count * LOC, ZM) * keep[lines]
        if half == 0:
            table_copy.wait()
            table = (table_ref[0], table_ref[1])
        for pair in range(LOC // 4):
            value = jnp.concatenate(
                [field[half, pl.ds(4 * pair + k, N, stride=LOC), :] for k in range(4)], axis=1
            )
            value = dot3(table, split(value))
            if half == 0:
                partial[pair] = value
            else:
                real = partial[pair, :N] - value[N:]
                imag = partial[pair, N:] + value[:N]
                for k in range(4):
                    lanes = slice(k * ZM, (k + 1) * ZM)
                    out[:, 0, 4 * pair + k] = real[:, lanes].reshape(GRID, LOC, ZM)
                    out[:, 1, 4 * pair + k] = imag[:, lanes].reshape(GRID, LOC, ZM)
                rows = pl.ds(4 * pair, 4)
                sent.append(pltpu.make_async_copy(out.at[:, :, rows], out_hbm.at[:, :, rows], sems.at[4, pair]))
                sent[-1].start()
    for copy in sent:
        copy.wait()


def plane_kernel(
    rank_ref, in_ref, noise_hbm, tables_hbm, out_ref, base, noise_ref, tables, sems
):
    step = pl.program_id(0)
    groups = LOC // STEP_PLANES
    table_copies = [
        pltpu.make_async_copy(tables_hbm.at[part], tables.at[part], sems.at[groups + k])
        for k, part in enumerate((pl.ds(0, 2), pl.ds(2, 2), pl.ds(4, 4)))
    ]

    def noise_copy(group):
        planes = pl.ds(group * STEP_PLANES, STEP_PLANES)
        return pltpu.make_async_copy(noise_hbm.at[0, :, planes], noise_ref.at[:, planes], sems.at[group])

    def to_field(group):
        lanes = []
        for inner in range(STEP_PLANES):
            rows = pl.ds(group * STEP_PLANES + inner, LOC, stride=LOC)
            real = jnp.concatenate([in_ref[g, 0, rows, :] for g in range(GRID)], axis=0)
            imag = jnp.concatenate([in_ref[g, 1, rows, :] for g in range(GRID)], axis=0)
            real, imag = column_transform((tables[0], tables[1]), real, imag)
            lanes.append(jnp.concatenate([real, imag], axis=1))
        value = split(jnp.concatenate(lanes, axis=0))
        parts = (pl.ds(0, N), pl.ds(N, N))
        return [dot3(value, (tables[2, lines], tables[3, lines])) for lines in parts]

    def from_field(group, field):
        lanes = []
        for inner in range(STEP_PLANES):
            plane = group * STEP_PLANES + inner
            pos_x = ((rank_ref[0] * LOC + plane).astype(F32) + 0.5) / N - 0.5
            shift_x = (TURN * trap_strength) * pos_x * pos_x
            real = field[0][inner * N : (inner + 1) * N]
            imag = field[1][inner * N : (inner + 1) * N]
            turns = (base[...] + shift_x) + (TURN * coupling) * (real * real + imag * imag)
            rest = turns - jnp.round(turns)
            square = rest * rest
            sine = polynomial(SIN_C, square) * rest
            cosine = polynomial(COS_C, square)
            decay = jnp.exp2(turns * DECAY_LOG2 + AMP_LOG2)
            evo_real = decay * (1.0 - sine * sine)
            evo_imag = decay * (sine * cosine)
            moved_real = real * evo_real + imag * evo_imag + noise_ref[0, plane]
            moved_imag = imag * evo_real - real * evo_imag + noise_ref[1, plane]
            lanes.append(jnp.concatenate([moved_real, moved_imag], axis=1))
        value = dot3(split(jnp.concatenate(lanes, axis=0)), (tables[4], tables[5]))
        for inner in range(STEP_PLANES):
            rows = pl.ds(group * STEP_PLANES + inner, LOC, stride=LOC)
            both = value[inner * N : (inner + 1) * N]
            real, imag = column_transform((tables[6], tables[7]), both[:, :ZM], both[:, ZM:])
            for g in range(GRID):
                out_ref[g, 0, rows, :] = real[g * LOC : (g + 1) * LOC]
                out_ref[g, 1, rows, :] = imag[g * LOC : (g + 1) * LOC]

    @pl.when(step == 0)
    def _():
        table_copies[0].start()
        table_copies[1].start()
        shape = (N, N)
        pos_y = (lax.broadcasted_iota(jnp.int32, shape, 0).astype(F32) + 0.5) / N - 0.5
        pos_z = (lax.broadcasted_iota(jnp.int32, shape, 1).astype(F32) + 0.5) / N - 0.5
        base[...] = TURN * (trap_strength * (pos_y * pos_y + pos_z * pos_z) - chem_potential)
        table_copies[0].wait()
        noise_copy(0).start()
        table_copies[2].start()
        table_copies[1].wait()
        for later in range(1, groups):
            noise_copy(later).start()

    field = to_field(step)
    noise_copy(step).wait()

    @pl.when(step == 0)
    def _():
        table_copies[2].wait()

    from_field(step, field)


def last_kernel(
    rank_ref, in_ref, mask_ref, table_ref, out_hbm, hist_ref, keep, field, occ, halves_ref, sems
):
    keep[...] = select_tiles(mask_ref[...]).astype(F32).reshape(N * LOC, ZM)
    lines = field.reshape(2, 2, N * LOC, ZM)
    half_rows = N // 2
    low_lane = lax.broadcasted_iota(jnp.int32, (half_rows, ZM), 1) < ZM // 2
    far = jnp.zeros((8, ZM), F32)
    mirror = lax.broadcasted_iota(jnp.int32, (NEAR, ZM), 1)
    low_near = mirror < ZM // 2
    mirror = jnp.where((mirror & (ZM // 2 - 1)) == 0, ZM // 2 - mirror, ZM - mirror)
    copies = []
    for upper in range(2):
        first = upper * half_rows
        table = tuple(
            jnp.concatenate(
                [table_ref[k, first : first + half_rows], table_ref[k, N + first : N + first + half_rows]], axis=0
            )
            for k in range(2)
        )
        even = None
        for row in range(LOC):
            if upper == 0:
                value = jnp.concatenate(
                    [in_ref[:, 0, row].reshape(N, ZM), in_ref[:, 1, row].reshape(N, ZM)], axis=1
                )
                held = split(value)
                halves_ref[row, 0] = held[0]
                halves_ref[row, 1] = held[1]
            else:
                held = halves_ref[row, 0], halves_ref[row, 1]
            both = dot3(table, held)
            real = both[:half_rows, :ZM] - both[half_rows:, ZM:]
            imag = both[:half_rows, ZM:] + both[half_rows:, :ZM]
            rows = pl.ds(first * LOC + row, half_rows, stride=LOC)
            mask = keep[rows, :]
            real = real * mask
            imag = imag * mask
            for half, value in enumerate((real, imag)):
                lines[half, 0, rows, :] = jnp.where(low_lane, value, 0.0)
                lines[half, 1, rows, :] = jnp.where(low_lane, 0.0, value)
            occupation = real * real + imag * imag
            if upper == 0:
                near, rest = occupation[:NEAR], occupation[NEAR:]
            else:
                rest, near = occupation[: half_rows - NEAR], occupation[half_rows - NEAR :]
            far = far + jnp.sum(rest.reshape(-1, 8, ZM), axis=0)
            if row % 2 == 0:
                even = near
                continue
            folded = jnp.where(low_near, even, near) + jnp.take_along_axis(
                jnp.where(low_near, near, even), mirror, axis=1, mode="promise_in_bounds"
            )
            high, low = split(folded)
            lanes = slice(row // 2 * ZM, (row // 2 + 1) * ZM)
            occ[upper * NEAR : (upper + 1) * NEAR, lanes] = high
            occ[(2 + upper) * NEAR : (3 + upper) * NEAR, lanes] = low
        part = pl.ds(first, half_rows)
        for half in range(2):
            for tile in range(2):
                copies.append(
                    pltpu.make_async_copy(
                        field.at[half, tile, part],
                        out_hbm.at[0, half, part, :, pl.ds(tile * ZM, ZM)],
                        sems.at[half, 2 * upper + tile],
                    )
                )
                copies[-1].start()

    shape = (LOC * ZM // 2, SHELLS)
    place = lax.broadcasted_iota(jnp.int32, shape, 0)
    lane = place & (ZM - 1)
    index_y = rank_ref[0] * LOC + 2 * (place >> 7) + (lane >> 6)
    sig_y = jnp.where(index_y < N // 2, index_y, index_y - N)
    sig_z = jnp.where(lane < ZM // 2, lane, (ZM - lane) & (ZM // 2 - 1))
    rest = jnp.minimum(sig_y * sig_y + sig_z * sig_z, 64 * (SHELLS - 1))
    gap = (rest - 64 * lax.broadcasted_iota(jnp.int32, shape, 1)).astype(F32)
    gap = jnp.clip(gap, -GAP_MAX, GAP_MAX).astype(BF16)
    count = 2 * NEAR
    shape = (count, SHELLS)
    index_x = lax.broadcasted_iota(jnp.int32, shape, 0)
    sig_x = jnp.where(index_x < NEAR, index_x, index_x - count)
    square_x = sig_x * sig_x
    residue = square_x & 63
    sums = jnp.zeros(shape, F32)
    one = jnp.ones((), BF16)
    zero = jnp.zeros((), BF16)
    for first in range(0, len(RESIDUES), 2):
        pair = RESIDUES[first : first + 2]
        hits = jnp.concatenate(
            [jnp.where(jnp.abs(gap + BF16(r - 31.5)) < BF16(32.0), one, zero) for r in pair], axis=1
        )
        found = dot(occ[...], hits)
        found = found[:count] + found[count:]
        for place_of, r in enumerate(pair):
            sums = jnp.where(residue == r, found[:, place_of * SHELLS : (place_of + 1) * SHELLS], sums)
    moves = square_x >> 6
    bins = lax.broadcasted_iota(jnp.int32, shape, 1)
    beyond = moves >= SHELLS - 1
    over = jnp.where(beyond, sums, 0.0)
    sums = jnp.where(beyond, 0.0, sums)
    for bit in range(7):
        width = 1 << bit
        chosen = (moves & width) != 0
        past = chosen & (bins >= SHELLS - width)
        over = over + jnp.where(past, sums, 0.0)
        rolled = jnp.where(bins >= width, pltpu.roll(sums, width, 1), 0.0)
        sums = jnp.where(chosen, rolled, sums)
    total = jnp.sum(sums, axis=0, keepdims=True)
    extra = jnp.sum(over, axis=0, keepdims=True) + jnp.sum(far, axis=0, keepdims=True)
    extra = jnp.sum(extra, axis=1, keepdims=True)
    hist = total + jnp.where(bins[:1] == SHELLS - 1, extra, 0.0)
    hist_ref[...] = jnp.broadcast_to(hist.reshape(1, 1, SHELLS), (GRID, 1, SHELLS))
    for copy in copies:
        copy.wait()


def params(mib):
    return pltpu.CompilerParams(vmem_limit_bytes=mib * 1024 * 1024)


def whole(shape):
    return pl.BlockSpec(shape, lambda *_: (0,) * len(shape))


def exchange(value):
    return lax.all_to_all(value, "grid", split_axis=0, concat_axis=0, tiled=True)


def shards(psi_modes, noise, mask):
    inv_tall, fwd_tall, inv_z, fwd_z = (halves(table) for table in host_tables())
    tables = jnp.asarray(np.concatenate([inv_tall, inv_z, fwd_z, fwd_tall]))
    rank = lax.axis_index("grid").astype(jnp.int32).reshape(1)
    smem = pl.BlockSpec(memory_space=pltpu.SMEM)
    hbm = pl.BlockSpec(memory_space=pltpu.HBM)
    message = (GRID, 2, LOC, LOC, ZM)
    flat = (GRID, 2, LOC * LOC, ZM)
    sent = pl.pallas_call(
        first_kernel,
        out_shape=jax.ShapeDtypeStruct(message, F32),
        grid=(1,),
        in_specs=[hbm] * 3,
        out_specs=hbm,
        scratch_shapes=[
            pltpu.VMEM((2, N, LOC, N), F32),
            pltpu.VMEM((N, LOC, N), jnp.int32),
            pltpu.VMEM((2, 2 * N, N), BF16),
            pltpu.VMEM((N * LOC, ZM), F32),
            pltpu.VMEM((2, N * LOC, ZM), F32),
            pltpu.VMEM((LOC // 4, 2 * N, 4 * ZM), F32),
            pltpu.VMEM(message, F32),
            pltpu.SemaphoreType.DMA((5, 4)),
        ],
        compiler_params=params(63),
        name="first",
    )(psi_modes, mask, tables)
    planes = exchange(sent).reshape(flat)
    sent = pl.pallas_call(
        plane_kernel,
        out_shape=jax.ShapeDtypeStruct(flat, F32),
        grid=(LOC // STEP_PLANES,),
        in_specs=[
            smem,
            whole(flat),
            hbm,
            hbm,
        ],
        out_specs=whole(flat),
        scratch_shapes=[
            pltpu.VMEM((N, N), F32),
            pltpu.VMEM((2, LOC, N, N), F32),
            pltpu.VMEM(tables.shape, BF16),
            pltpu.SemaphoreType.DMA((LOC // STEP_PLANES + 3,)),
        ],
        compiler_params=params(PLANES_MIB),
        name="planes",
    )(rank, planes, noise, tables)
    rows_in = exchange(sent).reshape(message)
    psi_next, hist = pl.pallas_call(
        last_kernel,
        out_shape=(
            jax.ShapeDtypeStruct(psi_modes.shape, F32),
            jax.ShapeDtypeStruct((GRID, 1, SHELLS), F32),
        ),
        grid=(1,),
        in_specs=[smem, whole(message), whole((N, LOC, N)), pl.BlockSpec((2, 2 * N, N), lambda i: (3, 0, 0))],
        out_specs=(hbm, whole((GRID, 1, SHELLS))),
        scratch_shapes=[
            pltpu.VMEM((N * LOC, ZM), F32),
            pltpu.VMEM((2, 2, N, LOC, ZM), F32),
            pltpu.VMEM((4 * NEAR, LOC * ZM // 2), BF16),
            pltpu.VMEM((LOC, 2, N, 2 * ZM), BF16),
            pltpu.SemaphoreType.DMA((2, 4)),
        ],
        compiler_params=params(24),
        name="last",
    )(rank, rows_in, mask, tables)
    hist = jnp.sum(exchange(hist), axis=0)
    other = [lax.ppermute(hist, "traj", [(t, (t + k) % TRAJ) for t in range(TRAJ)]) for k in (1, 2, 3)]
    hist = (hist + other[1]) + (other[0] + other[2])
    return psi_next, hist.reshape(SHELLS) * (SHELLS / (TRAJ * N * N * N))


def solution(mesh):
    placed = (
        P("traj", None, None, "grid", None),
        P("traj", None, "grid", None, None),
        P(None, "grid", None),
    )
    return jax.shard_map(
        shards,
        mesh=mesh,
        in_specs=placed,
        out_specs=(P("traj", None, None, "grid", None), P()),
        check_vma=False,
    )
```
